512 devices in a mesh: dp: 8 (over x, core), expert: 64 (over y, z).
Axes of the slice: x: 4, y: 8, z: 8, core: 2. Of those that a mesh axis runs over, the one named last changes fastest.
Arguments:
- cotangent: bfloat16 [65536, 3584], P(('dp', 'expert')), may hold values from -0.59765625 to 0.59765625
- expert_ids: int32 [65536, 1], P(('dp', 'expert')), may hold values from 0 to 15; in each aligned block of 128 rows (0 to 127, 128 to 255, ...) at most 12 rows name the same one
- route_weights: float32 [65536, 1], P(('dp', 'expert')), may hold values from 0.1 to 1
- gate_pre: bfloat16 [6144, 16384], P('dp', 'expert'), may hold values from -5 to 5
- up_pre: bfloat16 [6144, 16384], P('dp', 'expert'), may hold values from -5 to 5
- down_weight: bfloat16 [3584, 16384], P('dp', 'expert'), may hold values from -0.1875 to 0.1875
Outputs:
- weight_grad: bfloat16 [3584, 16384], P('dp', 'expert')
- gate_grad: bfloat16 [6144, 16384], P('dp', 'expert')
- up_grad: bfloat16 [6144, 16384], P('dp', 'expert')
The draws below stay inside these ranges and needn't reach their ends.
Inputs may be any that keep to these rules, and one draw needn't show every extreme that they name: `expert_ids`: each token names one expert. Among the tokens of one device, at most 12 name the same expert, and in every draw some expert is named by exactly 12 tokens of some device.
All inputs are finite; a program needn't handle non-finite values.
Results may differ from the reference program's by a relative error of at most 0.013.
Values may be sent and summed in bfloat16 or wider, within the bound.
A program may use at most 64 MiB of HBM per device.

```python
import math
import jax
import jax.numpy as jnp
import numpy as np
from jax import lax

D = 3584
FFW = 1024
TOP = 1
TOK_DEV = 128
EXPERTS = 16
CAP = 12
TOKENS = 65536
SLOTS = 6144
N_DP = 8
N_EXPERT = 64


def shard_levels(own_key, extent, split, low, largest):
    def one(axis_at, parts):
        steps = jax.random.uniform(jax.random.fold_in(jax.random.fold_in(own_key, 6), axis_at), (parts,), jnp.float32, low / len(split), largest / len(split))
        return jnp.repeat(jnp.exp(steps), extent[axis_at] // parts).reshape((-1,) + (1,) * (len(extent) - axis_at - 1))

    gain = one(*split[0])
    for cut in split[1:]:
        gain = gain * one(*cut)
    return gain


def assign_block(own_key, own, number, rows, count, top, limit, skew):
    order = jax.random.permutation(own_key, count)
    heavy_load, common = load_shares(count, rows * top, limit, skew, True), load_shares(count, rows * top, limit, skew, False)
    places = jnp.arange(count)

    def named(lengths, turn):
        used = int((lengths > 0).sum())
        fixed = max(1, used // 4)
        shifted = fixed + (places - fixed + turn * (used - fixed)) % max(1, count - fixed)
        return jnp.zeros((count,), jnp.int32).at[order[jnp.where(places < fixed, places, shifted)]].set(jnp.asarray(lengths, jnp.int32))

    lengths = jnp.where(number % 4 == 0, named(heavy_load, number // 4), named(common, number - number // 4 - 1))
    mixed = jax.random.permutation(jax.random.fold_in(own, 3), count)
    source_of, receiver = mixed[0:count // 2 * 2:2], mixed[1:count // 2 * 2:2]
    room = jnp.minimum(lengths[source_of] - 1, limit - lengths[receiver]) // 2
    room = jnp.where((source_of == order[0]) | (receiver == order[0]) | (lengths[receiver] == 0), 0, jnp.maximum(room, 0))
    shifted = jax.random.randint(jax.random.fold_in(own, 4), (count // 2,), 0, 1 << 20) % (room + 1)
    lengths = lengths.at[source_of].add(-shifted).at[receiver].add(shifted)
    labels = jnp.searchsorted(jnp.cumsum(lengths), jnp.arange(rows * top), side="right").astype(jnp.int32)
    listing = labels.reshape(top, rows).T
    listing = listing[jax.random.permutation(jax.random.fold_in(own, 1), rows)]
    turn = jax.random.randint(jax.random.fold_in(own, 2), (rows, 1), 0, top)
    return jnp.take_along_axis(listing, (jnp.arange(top)[None, :] + turn) % top, axis=1)


def load_shares(count, total, most, lean, full):
    weights = [(1 << 20) // math.isqrt(standing ** lean) + 1 for standing in range(1, count + 1)]
    largest = most if full else min(most, max(-(-total // count), total * weights[0] // sum(weights)))
    least = 1 if total - largest >= count - 1 else 0
    holding, surplus = [largest] + [least] * (count - 1), total - largest - least * (count - 1)
    while surplus > 0:
        movable = [i for i in range(1, count) if holding[i] < largest] or [i for i in range(1, count) if holding[i] < most]
        whole, left = sum([weights[i] for i in movable]), surplus
        for i in movable:
            more = min(most - holding[i], max(1, left * weights[i] // whole), surplus)
            holding[i] = holding[i] + more
            surplus = surplus - more
    return np.array(holding)


def normal_values(rng, extent, width, limit, cuts=(), kind=jnp.bfloat16):
    drawn = width * jax.random.normal(rng, extent, jnp.float32)
    if cuts:
        drawn = drawn * shard_levels(rng, extent, cuts, -0.22, 0.18)
    return jnp.clip(drawn, -limit, limit).astype(kind)


def setup_inputs(seed: int = 0) -> dict:
    splits = jax.random.split(jax.random.key(seed), 7)
    cotangent = normal_values(splits[0], (TOKENS, D), 0.1, 0.59765625, ((0, 512),))
    expert_ids_keys = jax.random.split(jax.random.fold_in(splits[1], 1), TOKENS // TOK_DEV)
    expert_ids_turns = jax.random.permutation(jax.random.fold_in(splits[1], 3), TOKENS // TOK_DEV)
    expert_ids = jax.vmap(lambda own, number: assign_block(jax.random.fold_in(splits[1], 2), own, number, TOK_DEV, EXPERTS, TOP, CAP, 2))(expert_ids_keys, expert_ids_turns).reshape((TOKENS, TOP))
    route_weights = jnp.clip(0.1 + 0.9 * jax.random.uniform(splits[2], (TOKENS, TOP), jnp.float32) ** shard_levels(splits[2], (TOKENS, TOP), ((0, 512),), -0.2, 0.2), 0.1, 1.0)
    gate_pre = normal_values(splits[3], (SLOTS, EXPERTS * FFW), 1.0, 5.0, ((0, 8), (1, 64)))
    up_pre = normal_values(splits[4], (SLOTS, EXPERTS * FFW), 1.0, 5.0, ((0, 8), (1, 64)))
    down_weight = normal_values(splits[5], (D, EXPERTS * FFW), FFW ** -0.5, 0.1875, ((0, 8), (1, 64)))
    return {"cotangent": cotangent, "expert_ids": expert_ids, "route_weights": route_weights, "gate_pre": gate_pre, "up_pre": up_pre, "down_weight": down_weight}


def group_terms(cotangent, expert_ids, route_weights, gate_pre, up_pre, down_weight):
    onehot = (expert_ids[..., None] == jnp.arange(EXPERTS, dtype=jnp.int32)).astype(jnp.int32)
    touched = jnp.sum(onehot, axis=2)
    earlier = jnp.cumsum(touched, axis=1) - touched
    position = jnp.sum(onehot * earlier[:, :, None, :], axis=3)
    sources = jnp.arange(N_EXPERT, dtype=jnp.int32)[:, None, None] * CAP
    rows = (sources + position).astype(jnp.int32)
    scaled = route_weights[..., None] * cotangent.astype(jnp.float32)[:, :, None, :]
    routed = jnp.zeros((EXPERTS, N_EXPERT * CAP, D), jnp.float32).at[expert_ids, rows].add(scaled)
    routed_half = lax.optimization_barrier(routed.astype(jnp.bfloat16))
    routed_full = routed_half.astype(jnp.float32)
    weights = down_weight.astype(jnp.float32).reshape(D, EXPERTS, FFW)
    gate_full = gate_pre.astype(jnp.float32).reshape(N_EXPERT * CAP, EXPERTS, FFW)
    up_full = up_pre.astype(jnp.float32).reshape(N_EXPERT * CAP, EXPERTS, FFW)
    upstream = jnp.einsum('xrd,dxf->rxf', routed_full, weights)
    sigmoid = jax.nn.sigmoid(gate_full)
    active = gate_full * sigmoid
    product_half = lax.optimization_barrier((active * up_full).astype(jnp.bfloat16))
    gate_grad = (upstream * up_full * sigmoid * (1.0 + gate_full * (1.0 - sigmoid))).astype(jnp.bfloat16)
    up_grad = (upstream * active).astype(jnp.bfloat16)
    partial_sum = jnp.einsum('xrd,rxf->dxf', routed_full, product_half.astype(jnp.float32))
    partial_half = partial_sum.reshape(D, EXPERTS * FFW).astype(jnp.bfloat16)
    return partial_half, gate_grad.reshape(N_EXPERT * CAP, EXPERTS * FFW), up_grad.reshape(N_EXPERT * CAP, EXPERTS * FFW)


def reference(cotangent, expert_ids, route_weights, gate_pre, up_pre, down_weight):
    stacked = (cotangent.reshape(N_DP, N_EXPERT, TOK_DEV, D),
               expert_ids.reshape(N_DP, N_EXPERT, TOK_DEV, TOP),
               route_weights.reshape(N_DP, N_EXPERT, TOK_DEV, TOP),
               gate_pre.reshape(N_DP, N_EXPERT * CAP, EXPERTS * FFW),
               up_pre.reshape(N_DP, N_EXPERT * CAP, EXPERTS * FFW))

    def step(total, pieces):
        partial_half, gate_grad, up_grad = group_terms(pieces[0], pieces[1], pieces[2], pieces[3], pieces[4], down_weight)
        return total + partial_half.astype(jnp.float32), (gate_grad, up_grad)

    start = jnp.zeros((D, EXPERTS * FFW), jnp.float32)
    total, grads = lax.scan(step, start, stacked)
    weight_grad = total.astype(jnp.bfloat16)
    gate_grad = grads[0].reshape(SLOTS, EXPERTS * FFW)
    up_grad = grads[1].reshape(SLOTS, EXPERTS * FFW)
    return weight_grad, gate_grad, up_grad
```

```python
import jax
import jax.numpy as jnp
from jax import lax
from jax.sharding import PartitionSpec as P

SPLIT = 4


def slot_buffer(cotangent, expert_ids, route_weights, experts, capacity):
    columns = lax.broadcasted_iota(jnp.int32, (1, 1, experts), 2)
    onehot = (expert_ids[:, :, None] == columns).astype(jnp.int32)
    touched = jnp.sum(onehot, axis=1)
    earlier = jnp.cumsum(touched, axis=0) - touched
    position = jnp.sum(onehot * earlier[:, None, :], axis=2)
    target = expert_ids * capacity + position
    places = lax.broadcasted_iota(jnp.int32, (1, 1, experts * capacity), 2)
    chosen = (target[:, :, None] == places).astype(jnp.float32)
    picker = jnp.sum(chosen, axis=1)
    slot_scale = jnp.sum(chosen * route_weights[:, :, None], axis=(0, 1))
    picked = lax.dot_general(
        picker.astype(jnp.bfloat16),
        cotangent,
        (((0,), (0,)), ((), ())),
        preferred_element_type=jnp.float32,
    )
    return (picked * slot_scale[:, None]).astype(jnp.bfloat16)


def per_device(cotangent, expert_ids, route_weights, gate_pre, up_pre, down_weight):
    devices = lax.axis_size("expert")
    groups = lax.axis_size("dp")
    experts = devices // SPLIT
    rows, hidden = gate_pre.shape
    capacity = rows // devices
    width = cotangent.shape[1]
    part = width // SPLIT
    piece = part // groups
    quads = [[x * SPLIT + q for q in range(SPLIT)] for x in range(experts)]

    def quad_exchange(array):
        return lax.all_to_all(
            array, "expert", split_axis=0, concat_axis=0, axis_index_groups=quads, tiled=True
        )

    gate = gate_pre.astype(jnp.float32)
    up = up_pre.astype(jnp.float32)
    sigmoid = jax.nn.sigmoid(gate)
    active = gate * sigmoid
    product = (active * up).astype(jnp.bfloat16)

    ordered = cotangent.reshape(-1, groups, SPLIT, piece).transpose(0, 2, 1, 3).reshape(-1, width)
    buffer = slot_buffer(ordered, expert_ids, route_weights, experts, capacity)
    sent = buffer.reshape(experts, capacity // 4, 4, SPLIT, part).transpose(0, 3, 1, 2, 4)
    arrived = lax.all_to_all(
        sent.reshape(devices, capacity // 4, 4, part),
        "expert",
        split_axis=0,
        concat_axis=0,
        tiled=True,
    )
    routed = arrived.reshape(rows, part)

    weight = quad_exchange(down_weight.reshape(SPLIT, piece, hidden))
    weight = lax.all_to_all(
        jnp.broadcast_to(weight, (groups, *weight.shape)), "dp", split_axis=0, concat_axis=0, tiled=True
    )
    weight = weight.transpose(1, 0, 2, 3).reshape(SPLIT, part, hidden)
    products = quad_exchange(jnp.broadcast_to(product, (SPLIT, *product.shape)))

    partial = jnp.einsum("rd,jdf->jrf", routed, weight, preferred_element_type=jnp.float32)
    shares = quad_exchange(partial.astype(jnp.bfloat16))
    upstream = shares.astype(jnp.float32).sum(axis=0)
    gate_grad = (upstream * up * sigmoid * (1.0 + gate * (1.0 - sigmoid))).astype(jnp.bfloat16)
    up_grad = (upstream * active).astype(jnp.bfloat16)

    grads = jnp.einsum("rd,jrf->djf", routed, products, preferred_element_type=jnp.float32)
    grads = grads.astype(jnp.bfloat16).reshape(groups, piece, SPLIT, hidden)
    grads = lax.all_to_all(grads, "dp", split_axis=0, concat_axis=0, tiled=True)
    total = grads.astype(jnp.float32).sum(axis=0).astype(jnp.bfloat16)
    weight_grad = quad_exchange(total.transpose(1, 0, 2)).reshape(SPLIT * piece, hidden)
    return (weight_grad, gate_grad, up_grad)


def solution(mesh):
    placed = (
        P(("dp", "expert"), None),
        P(("dp", "expert"), None),
        P(("dp", "expert"), None),
        P("dp", "expert"),
        P("dp", "expert"),
        P("dp", "expert"),
    )
    return jax.shard_map(
        per_device,
        mesh=mesh,
        in_specs=placed,
        out_specs=(P("dp", "expert"), P("dp", "expert"), P("dp", "expert")),
        check_vma=False,
    )
```

```python
import functools

import jax
import jax.numpy as jnp
from jax import lax
from jax.experimental import pallas as pl
from jax.experimental.pallas import tpu as pltpu
from jax.sharding import PartitionSpec as P

SPLIT = 4
MESH = pl.DeviceIdType.MESH


def slot_buffer(cotangent, expert_ids, route_weights, experts, capacity):
    columns = lax.broadcasted_iota(jnp.int32, (1, 1, experts), 2)
    onehot = (expert_ids[:, :, None] == columns).astype(jnp.int32)
    touched = jnp.sum(onehot, axis=1)
    earlier = jnp.cumsum(touched, axis=0) - touched
    position = jnp.sum(onehot * earlier[:, None, :], axis=2)
    target = expert_ids * capacity + position
    places = lax.broadcasted_iota(jnp.int32, (1, 1, experts * capacity), 2)
    chosen = (target[:, :, None] == places).astype(jnp.float32)
    picker = jnp.sum(chosen, axis=1)
    slot_scale = jnp.sum(chosen * route_weights[:, :, None], axis=(0, 1))
    picked = lax.dot_general(
        picker.astype(jnp.bfloat16),
        cotangent,
        (((0,), (0,)), ((), ())),
        preferred_element_type=jnp.float32,
    )
    return (picked * slot_scale[:, None]).astype(jnp.bfloat16)


def wait_bytes(ref, sem):
    pltpu.make_async_copy(ref, ref, sem).wait()


def layer_kernel(
    dims,
    sent,
    gate,
    up,
    down,
    weight_grad,
    gate_grad,
    up_grad,
    arrived,
    routed,
    own_weight,
    weight,
    products,
    partial,
    shares,
    grads,
    grad_parts,
    total,
    grad_rows,
    send_sems,
    token_sems,
    quad_weight_sems,
    weight_sems,
    product_sems,
    share_sems,
    grad_sems,
    total_sems,
):
    groups, devices, ring = dims
    rows_y = devices // ring
    rows, hidden = gate.shape
    capacity = rows // devices
    chunk = rows // rows_y
    piece = down.shape[0] // SPLIT
    part = piece * groups
    i = lax.axis_index("dp")
    e = lax.axis_index("expert")
    y, z = e // ring, e % ring
    q = e % SPLIT
    base = e - q

    def peer(target):
        return {"expert": target}

    barrier = pltpu.get_barrier_semaphore()

    @pl.loop(1, devices)
    def _(step):
        target = lax.rem(e + step, devices)
        pl.semaphore_signal(barrier, inc=1, device_id=peer(target), device_id_type=MESH)

    @pl.loop(1, groups)
    def _(step):
        target = lax.rem(i + step, groups)
        pl.semaphore_signal(barrier, inc=1, device_id={"dp": target}, device_id_type=MESH)

    arrived[e] = sent[e]
    own_weight[q] = down[pl.ds(pl.multiple_of(q * piece, 16), piece), :]
    pl.semaphore_wait(barrier, devices - 1 + groups - 1)

    for step in range(1, SPLIT):
        other = lax.rem(q + step, SPLIT)
        pltpu.make_async_remote_copy(
            src_ref=down.at[pl.ds(pl.multiple_of(other * piece, 16), piece)],
            dst_ref=own_weight.at[q],
            send_sem=send_sems.at[0],
            recv_sem=quad_weight_sems.at[q],
            device_id=peer(base + other),
            device_id_type=MESH,
        ).start()

    def away(step, count):
        return jnp.where(step % 2 == 1, (step + 1) // 2, count - step // 2)

    @pl.loop(0, devices)
    def _(step):
        to_y = lax.rem(y + away(step // ring, rows_y), rows_y)
        to_z = lax.rem(z + away(step % ring, ring), ring)
        target = to_y * ring + to_z

        @pl.when(target != e)
        def _():
            pltpu.make_async_remote_copy(
                src_ref=sent.at[target],
                dst_ref=arrived.at[e],
                send_sem=send_sems.at[1],
                recv_sem=token_sems.at[e],
                device_id=peer(target),
                device_id_type=MESH,
            ).start()

    @pl.loop(0, rows_y)
    def _(step):
        span = pl.ds(pl.multiple_of(step * chunk, 16), chunk)
        g = gate[span, :].astype(jnp.float32)
        active = g / (1.0 + jnp.exp(-g))
        products[q, span, :] = (active * up[span, :].astype(jnp.float32)).astype(jnp.bfloat16)

    for step in range(1, SPLIT):
        other = lax.rem(q + step, SPLIT)
        wait_bytes(own_weight.at[other], quad_weight_sems.at[other])
    weight[i] = own_weight[...]

    @pl.loop(1, groups)
    def _(step):
        target = lax.rem(i + step, groups)
        pltpu.make_async_remote_copy(
            src_ref=own_weight,
            dst_ref=weight.at[i],
            send_sem=send_sems.at[2],
            recv_sem=weight_sems.at[i],
            device_id={"dp": target},
            device_id_type=MESH,
        ).start()

    for step in range(1, SPLIT):
        other = lax.rem(q + step, SPLIT)
        pltpu.make_async_remote_copy(
            src_ref=products.at[q],
            dst_ref=products.at[q],
            send_sem=send_sems.at[3],
            recv_sem=product_sems.at[q],
            device_id=peer(base + other),
            device_id_type=MESH,
        ).start()

    @pl.loop(1, groups)
    def _(step):
        source = lax.rem(i + step, groups)
        wait_bytes(weight.at[source], weight_sems.at[source])

    @pl.loop(0, rows_y)
    def _(step):
        from_y = lax.rem(y + rows_y - lax.rem(away(step, rows_y), rows_y), rows_y)

        @pl.loop(0, ring)
        def _(at):
            source = from_y * ring + at

            @pl.when(source != e)
            def _():
                wait_bytes(arrived.at[source], token_sems.at[source])

        block = arrived[pl.ds(from_y * ring, ring)].reshape(chunk, part)
        span = pl.ds(pl.multiple_of(from_y * chunk, 16), chunk)
        routed[span, :] = block
        for j in range(SPLIT):
            partial[j, span, :] = jnp.dot(
                block, weight[:, j].reshape(part, hidden), preferred_element_type=jnp.float32
            ).astype(jnp.bfloat16)
        shares[q, span, :] = partial[q, span, :]
        for hop in range(1, SPLIT):
            other = lax.rem(q + hop, SPLIT)
            pltpu.make_async_remote_copy(
                src_ref=partial.at[other, span],
                dst_ref=shares.at[q, span],
                send_sem=send_sems.at[4],
                recv_sem=share_sems.at[q, from_y],
                device_id=peer(base + other),
                device_id_type=MESH,
            ).start()

    for step in range(1, SPLIT):
        other = lax.rem(q + step, SPLIT)
        wait_bytes(products.at[other], product_sems.at[other])

    @pl.loop(0, SPLIT)
    def _(j):
        grads[:, j] = (
            lax.dot_general(
                routed[...],
                products[j],
                (((0,), (0,)), ((), ())),
                preferred_element_type=jnp.float32,
            )
            .astype(jnp.bfloat16)
            .reshape(groups, piece, hidden)
        )

    grad_parts[i] = grads[i]

    @pl.loop(1, groups)
    def _(step):
        target = lax.rem(i + step, groups)
        pltpu.make_async_remote_copy(
            src_ref=grads.at[target],
            dst_ref=grad_parts.at[i],
            send_sem=send_sems.at[5],
            recv_sem=grad_sems.at[i],
            device_id={"dp": target},
            device_id_type=MESH,
        ).start()

    @pl.loop(0, rows_y)
    def _(step):
        from_y = lax.rem(y + rows_y - lax.rem(away(step, rows_y), rows_y), rows_y)
        span = pl.ds(pl.multiple_of(from_y * chunk, 16), chunk)
        for hop in range(1, SPLIT):
            other = lax.rem(q + hop, SPLIT)
            wait_bytes(shares.at[other, span], share_sems.at[other, from_y])
        upstream = shares[0, span, :].astype(jnp.float32)
        for j in range(1, SPLIT):
            upstream = upstream + shares[j, span, :].astype(jnp.float32)
        g = gate[span, :].astype(jnp.float32)
        u = up[span, :].astype(jnp.float32)
        sigmoid = 1.0 / (1.0 + jnp.exp(-g))
        gate_grad[span, :] = (upstream * u * sigmoid * (1.0 + g * (1.0 - sigmoid))).astype(
            jnp.bfloat16
        )
        up_grad[span, :] = (upstream * (g * sigmoid)).astype(jnp.bfloat16)

    @pl.loop(1, groups)
    def _(step):
        source = lax.rem(i + step, groups)
        wait_bytes(grad_parts.at[source], grad_sems.at[source])

    @pl.loop(0, SPLIT)
    def _(j):
        whole = grad_parts[0, j].astype(jnp.float32)
        for k in range(1, groups):
            whole = whole + grad_parts[k, j].astype(jnp.float32)
        total[j] = whole.astype(jnp.bfloat16)

    grad_rows[q] = total[q]
    for step in range(1, SPLIT):
        other = lax.rem(q + step, SPLIT)
        pltpu.make_async_remote_copy(
            src_ref=total.at[other],
            dst_ref=grad_rows.at[q],
            send_sem=send_sems.at[6],
            recv_sem=total_sems.at[q],
            device_id=peer(base + other),
            device_id_type=MESH,
        ).start()
    for step in range(1, SPLIT):
        other = lax.rem(q + step, SPLIT)
        wait_bytes(grad_rows.at[other], total_sems.at[other])
    for j in range(SPLIT):
        weight_grad[j * piece : (j + 1) * piece, :] = grad_rows[j]

    wait_bytes(own_weight.at[pl.ds(0, SPLIT - 1)], send_sems.at[0])
    wait_bytes(arrived.at[pl.ds(0, devices - 1)], send_sems.at[1])
    wait_bytes(weight.at[pl.ds(0, groups - 1)], send_sems.at[2])
    wait_bytes(products.at[pl.ds(0, SPLIT - 1)], send_sems.at[3])
    wait_bytes(shares.at[pl.ds(0, SPLIT - 1)], send_sems.at[4])
    wait_bytes(grads.at[pl.ds(0, groups - 1)], send_sems.at[5])
    wait_bytes(total.at[pl.ds(0, SPLIT - 1)], send_sems.at[6])


def per_device(cotangent, expert_ids, route_weights, gate_pre, up_pre, down_weight):
    devices = lax.axis_size("expert")
    groups = lax.axis_size("dp")
    ring = 8 if devices == 64 else SPLIT
    experts = devices // SPLIT
    rows, hidden = gate_pre.shape
    capacity = rows // devices
    width = cotangent.shape[1]
    part = width // SPLIT
    piece = part // groups

    ordered = cotangent.reshape(-1, groups, SPLIT, piece).transpose(0, 2, 1, 3).reshape(-1, width)
    buffer = slot_buffer(ordered, expert_ids, route_weights, experts, capacity)
    sent = buffer.reshape(experts, capacity // 4, 4, SPLIT, part).transpose(0, 3, 1, 2, 4)
    sent = sent.reshape(devices, capacity // 4, 4, part)

    half = jnp.bfloat16
    vmem = pl.BlockSpec(memory_space=pltpu.VMEM)
    dma = pltpu.SemaphoreType.DMA
    return pl.pallas_call(
        functools.partial(layer_kernel, (groups, devices, ring)),
        out_shape=(
            jax.ShapeDtypeStruct(down_weight.shape, half),
            jax.ShapeDtypeStruct(gate_pre.shape, half),
            jax.ShapeDtypeStruct(gate_pre.shape, half),
        ),
        in_specs=[vmem] * 4,
        out_specs=(vmem, vmem, vmem),
        scratch_shapes=[
            pltpu.VMEM((devices, capacity // 4, 4, part), half),
            pltpu.VMEM((rows, part), half),
            pltpu.VMEM((SPLIT, piece, hidden), half),
            pltpu.VMEM((groups, SPLIT, piece, hidden), half),
            pltpu.VMEM((SPLIT, rows, hidden), half),
            pltpu.VMEM((SPLIT, rows, hidden), half),
            pltpu.VMEM((SPLIT, rows, hidden), half),
            pltpu.VMEM((groups, SPLIT, piece, hidden), half),
            pltpu.VMEM((groups, SPLIT, piece, hidden), half),
            pltpu.VMEM((SPLIT, piece, hidden), half),
            pltpu.VMEM((SPLIT, piece, hidden), half),
            dma((7,)),
            dma((devices,)),
            dma((SPLIT,)),
            dma((groups,)),
            dma((SPLIT,)),
            dma((SPLIT, devices // ring)),
            dma((groups,)),
            dma((SPLIT,)),
        ],
        compiler_params=pltpu.CompilerParams(
            collective_id=0, has_side_effects=True, vmem_limit_bytes=48 * 1024 * 1024
        ),
    )(sent, gate_pre, up_pre, down_weight)


def solution(mesh):
    placed = (
        P(("dp", "expert"), None),
        P(("dp", "expert"), None),
        P(("dp", "expert"), None),
        P("dp", "expert"),
        P("dp", "expert"),
        P("dp", "expert"),
    )
    return jax.shard_map(
        per_device,
        mesh=mesh,
        in_specs=placed,
        out_specs=(P("dp", "expert"), P("dp", "expert"), P("dp", "expert")),
        check_vma=False,
    )
```

```python
import functools

import jax
import jax.numpy as jnp
from jax import lax
from jax.experimental import pallas as pl
from jax.experimental.pallas import tpu as pltpu
from jax.sharding import PartitionSpec as P

SPLIT = 4
PASS_ON = 2
MESH = pl.DeviceIdType.MESH


def fill_slots(groups, cotangent, ids, scales, ordered, sent):
    experts, _, quarters, lanes4, part = sent.shape
    tokens, width = cotangent.shape
    capacity = quarters * lanes4
    piece = part // groups
    lanes = 128 if part % 128 == 0 else part
    at = lax.broadcasted_iota(jnp.int32, (tokens, lanes), 1)
    for tile in range(width // lanes):
        whole = None
        lane = 0
        while lane < lanes:
            q, rest = divmod(tile * lanes + lane, part)
            i, t = divmod(rest, piece)
            source = i * SPLIT * piece + q * piece + t
            run = min(lanes - lane, piece - t, lanes - source % lanes)
            block = cotangent[:, source // lanes * lanes : (source // lanes + 1) * lanes]
            block = block.astype(jnp.float32)
            shift = (lane - source % lanes) % lanes
            if shift:
                block = pltpu.roll(block, shift, 1)
            whole = block if whole is None else jnp.where(at >= lane, block, whole)
            lane += run
        q, rest = divmod(tile * lanes, part)
        ordered[q, :, rest : rest + lanes] = whole.astype(jnp.bfloat16)

    names = ids[...]
    onehot = lax.broadcasted_iota(jnp.int32, (experts, tokens), 0) == names
    onehot = onehot.astype(jnp.float32)
    before = lax.broadcasted_iota(jnp.int32, (tokens, tokens), 0)
    before = before < lax.broadcasted_iota(jnp.int32, (tokens, tokens), 1)
    earlier = jnp.dot(
        onehot.astype(jnp.bfloat16),
        before.astype(jnp.float32).astype(jnp.bfloat16),
        preferred_element_type=jnp.float32,
    )
    position = jnp.sum(onehot * earlier, axis=0, keepdims=True)
    place = names.astype(jnp.float32) * capacity + position
    slots = lax.broadcasted_iota(jnp.int32, (experts * capacity, tokens), 0)
    picker = (slots.astype(jnp.float32) == place).astype(jnp.float32)
    slot_scale = jnp.sum(picker * scales[...], axis=1, keepdims=True)
    picker = picker.astype(jnp.bfloat16)
    for q in range(SPLIT):
        picked = jnp.dot(picker, ordered[q], preferred_element_type=jnp.float32)
        picked = (picked * slot_scale).astype(jnp.bfloat16)
        sent[:, q] = picked.reshape(experts, quarters, lanes4, part)


def wait_bytes(ref, sem):
    pltpu.make_async_copy(ref, ref, sem).wait()


def layer_kernel(
    dims,
    cotangent,
    ids,
    scales,
    gate,
    up,
    down,
    weight_grad,
    gate_grad,
    up_grad,
    ordered,
    sent,
    arrived,
    routed,
    own_weight,
    weight,
    products,
    partial,
    shares,
    grads,
    grad_parts,
    total,
    grad_rows,
    send_sems,
    token_sems,
    quad_weight_sems,
    weight_sems,
    product_sems,
    share_sems,
    grad_sems,
    total_sems,
):
    groups, devices, ring = dims
    rows_y = devices // ring
    rows, hidden = gate.shape
    capacity = rows // devices
    chunk = rows // rows_y
    piece = down.shape[0] // SPLIT
    part = piece * groups
    i = lax.axis_index("dp")
    e = lax.axis_index("expert")
    y, z = e // ring, e % ring
    q = e % SPLIT
    base = e - q

    def peer(target):
        return {"expert": target}

    barrier = pltpu.get_barrier_semaphore()

    @pl.loop(1, devices)
    def _(step):
        target = lax.rem(e + step, devices)
        pl.semaphore_signal(barrier, inc=1, device_id=peer(target), device_id_type=MESH)

    @pl.loop(1, groups)
    def _(step):
        target = lax.rem(i + step, groups)
        pl.semaphore_signal(barrier, inc=1, device_id={"dp": target}, device_id_type=MESH)

    fill_slots(groups, cotangent, ids, scales, ordered, sent)
    arrived[e] = sent[e // SPLIT, q]

    @pl.loop(0, rows_y)
    def _(step):
        span = pl.ds(pl.multiple_of(step * chunk, 16), chunk)
        g = gate[span, :].astype(jnp.float32)
        active = g / (1.0 + jnp.exp(-g))
        products[q, span, :] = (active * up[span, :].astype(jnp.float32)).astype(jnp.bfloat16)

    own_weight[q] = down[pl.ds(pl.multiple_of(q * piece, 16), piece), :]
    pl.semaphore_wait(barrier, devices - 1 + groups - 1)

    for step in range(1, SPLIT):
        other = lax.rem(q + step, SPLIT)
        pltpu.make_async_remote_copy(
            src_ref=down.at[pl.ds(pl.multiple_of(other * piece, 16), piece)],
            dst_ref=own_weight.at[q],
            send_sem=send_sems.at[0],
            recv_sem=quad_weight_sems.at[q],
            device_id=peer(base + other),
            device_id_type=MESH,
        ).start()

    inner = (q == 1) | (q == 2)

    def product_to(block, other, stage):
        pltpu.make_async_remote_copy(
            src_ref=products.at[block],
            dst_ref=products.at[block],
            send_sem=send_sems.at[stage],
            recv_sem=product_sems.at[block],
            device_id=peer(base + other),
            device_id_type=MESH,
        ).start()

    @pl.when(q < SPLIT - 1)
    def _():
        product_to(q, q + 1, 3)

    @pl.when(q > 0)
    def _():
        product_to(q, q - 1, 3)

    def away(step, count):
        return jnp.where(step % 2 == 1, (step + 1) // 2, count - step // 2)

    @pl.loop(0, devices)
    def _(step):
        to_y = lax.rem(y + away(step // ring, rows_y), rows_y)
        to_z = lax.rem(z + away(step % ring, ring), ring)
        target = to_y * ring + to_z

        @pl.when(target != e)
        def _():
            pltpu.make_async_remote_copy(
                src_ref=sent.at[target // SPLIT, target % SPLIT],
                dst_ref=arrived.at[e],
                send_sem=send_sems.at[1],
                recv_sem=token_sems.at[e],
                device_id=peer(target),
                device_id_type=MESH,
            ).start()

    for step in range(1, SPLIT):
        other = lax.rem(q + step, SPLIT)
        wait_bytes(own_weight.at[other], quad_weight_sems.at[other])
    weight[i] = own_weight[...]

    @pl.loop(1, groups)
    def _(step):
        target = lax.rem(i + step, groups)
        pltpu.make_async_remote_copy(
            src_ref=own_weight,
            dst_ref=weight.at[i],
            send_sem=send_sems.at[2],
            recv_sem=weight_sems.at[i],
            device_id={"dp": target},
            device_id_type=MESH,
        ).start()

    @pl.loop(1, groups)
    def _(step):
        source = lax.rem(i + step, groups)
        wait_bytes(weight.at[source], weight_sems.at[source])

    @pl.loop(0, rows_y)
    def _(step):
        from_y = lax.rem(y + rows_y - lax.rem(away(step, rows_y), rows_y), rows_y)

        @pl.loop(0, ring)
        def _(at):
            source = from_y * ring + at

            @pl.when(source != e)
            def _():
                wait_bytes(arrived.at[source], token_sems.at[source])

        @pl.when(inner & (step == min(PASS_ON, rows_y - 1)))
        def _():
            for way in (1, -1):
                wait_bytes(products.at[q - way], product_sems.at[q - way])
                product_to(q - way, q + way, 7)

        block = arrived[pl.ds(from_y * ring, ring)].reshape(chunk, part)
        span = pl.ds(pl.multiple_of(from_y * chunk, 16), chunk)
        routed[span, :] = block
        for j in range(SPLIT):
            partial[j, span, :] = jnp.dot(
                block, weight[:, j].reshape(part, hidden), preferred_element_type=jnp.float32
            ).astype(jnp.bfloat16)
        shares[q, span, :] = partial[q, span, :]
        for hop in range(1, SPLIT):
            other = lax.rem(q + hop, SPLIT)
            pltpu.make_async_remote_copy(
                src_ref=partial.at[other, span],
                dst_ref=shares.at[q, span],
                send_sem=send_sems.at[4],
                recv_sem=share_sems.at[q, from_y],
                device_id=peer(base + other),
                device_id_type=MESH,
            ).start()

    far = jnp.where(q == 1, SPLIT - 1, 0)

    @pl.when(inner)
    def _():
        wait_bytes(products.at[far], product_sems.at[far])
        product_to(far, jnp.where(q == 1, 0, SPLIT - 1), 8)

    @pl.when(jnp.logical_not(inner))
    def _():
        for step in range(1, SPLIT):
            other = lax.rem(q + step, SPLIT)
            wait_bytes(products.at[other], product_sems.at[other])

    @pl.loop(0, SPLIT)
    def _(j):
        grads[:, j] = (
            lax.dot_general(
                routed[...],
                products[j],
                (((0,), (0,)), ((), ())),
                preferred_element_type=jnp.float32,
            )
            .astype(jnp.bfloat16)
            .reshape(groups, piece, hidden)
        )

    grad_parts[i] = grads[i]

    @pl.loop(1, groups)
    def _(step):
        target = lax.rem(i + step, groups)
        pltpu.make_async_remote_copy(
            src_ref=grads.at[target],
            dst_ref=grad_parts.at[i],
            send_sem=send_sems.at[5],
            recv_sem=grad_sems.at[i],
            device_id={"dp": target},
            device_id_type=MESH,
        ).start()

    @pl.loop(0, rows_y)
    def _(step):
        from_y = lax.rem(y + rows_y - lax.rem(away(step, rows_y), rows_y), rows_y)
        span = pl.ds(pl.multiple_of(from_y * chunk, 16), chunk)
        for hop in range(1, SPLIT):
            other = lax.rem(q + hop, SPLIT)
            wait_bytes(shares.at[other, span], share_sems.at[other, from_y])
        upstream = shares[0, span, :].astype(jnp.float32)
        for j in range(1, SPLIT):
            upstream = upstream + shares[j, span, :].astype(jnp.float32)
        g = gate[span, :].astype(jnp.float32)
        u = up[span, :].astype(jnp.float32)
        sigmoid = 1.0 / (1.0 + jnp.exp(-g))
        gate_grad[span, :] = (upstream * u * sigmoid * (1.0 + g * (1.0 - sigmoid))).astype(
            jnp.bfloat16
        )
        up_grad[span, :] = (upstream * (g * sigmoid)).astype(jnp.bfloat16)

    @pl.loop(1, groups)
    def _(step):
        source = lax.rem(i + step, groups)
        wait_bytes(grad_parts.at[source], grad_sems.at[source])

    @pl.loop(0, SPLIT)
    def _(j):
        whole = grad_parts[0, j].astype(jnp.float32)
        for k in range(1, groups):
            whole = whole + grad_parts[k, j].astype(jnp.float32)
        total[j] = whole.astype(jnp.bfloat16)

    grad_rows[q] = total[q]
    for step in range(1, SPLIT):
        other = lax.rem(q + step, SPLIT)
        pltpu.make_async_remote_copy(
            src_ref=total.at[other],
            dst_ref=grad_rows.at[q],
            send_sem=send_sems.at[6],
            recv_sem=total_sems.at[q],
            device_id=peer(base + other),
            device_id_type=MESH,
        ).start()
    for step in range(1, SPLIT):
        other = lax.rem(q + step, SPLIT)
        wait_bytes(grad_rows.at[other], total_sems.at[other])
    for j in range(SPLIT):
        weight_grad[j * piece : (j + 1) * piece, :] = grad_rows[j]

    wait_bytes(own_weight.at[pl.ds(0, SPLIT - 1)], send_sems.at[0])
    wait_bytes(arrived.at[pl.ds(0, devices - 1)], send_sems.at[1])
    wait_bytes(weight.at[pl.ds(0, groups - 1)], send_sems.at[2])

    @pl.when(inner)
    def _():
        wait_bytes(products.at[pl.ds(0, 2)], send_sems.at[3])
        wait_bytes(products.at[pl.ds(0, 2)], send_sems.at[7])
        wait_bytes(products.at[0], send_sems.at[8])

    @pl.when(jnp.logical_not(inner))
    def _():
        wait_bytes(products.at[0], send_sems.at[3])

    wait_bytes(shares.at[pl.ds(0, SPLIT - 1)], send_sems.at[4])
    wait_bytes(grads.at[pl.ds(0, groups - 1)], send_sems.at[5])
    wait_bytes(total.at[pl.ds(0, SPLIT - 1)], send_sems.at[6])


def per_device(cotangent, expert_ids, route_weights, gate_pre, up_pre, down_weight):
    devices = lax.axis_size("expert")
    groups = lax.axis_size("dp")
    ring = 8 if devices == 64 else SPLIT
    experts = devices // SPLIT
    rows, hidden = gate_pre.shape
    capacity = rows // devices
    tokens, width = cotangent.shape
    part = width // SPLIT
    piece = part // groups

    half = jnp.bfloat16
    vmem = pl.BlockSpec(memory_space=pltpu.VMEM)
    dma = pltpu.SemaphoreType.DMA
    return pl.pallas_call(
        functools.partial(layer_kernel, (groups, devices, ring)),
        out_shape=(
            jax.ShapeDtypeStruct(down_weight.shape, half),
            jax.ShapeDtypeStruct(gate_pre.shape, half),
            jax.ShapeDtypeStruct(gate_pre.shape, half),
        ),
        in_specs=[vmem] * 6,
        out_specs=(vmem, vmem, vmem),
        scratch_shapes=[
            pltpu.VMEM((SPLIT, tokens, part), half),
            pltpu.VMEM((experts, SPLIT, capacity // 4, 4, part), half),
            pltpu.VMEM((devices, capacity // 4, 4, part), half),
            pltpu.VMEM((rows, part), half),
            pltpu.VMEM((SPLIT, piece, hidden), half),
            pltpu.VMEM((groups, SPLIT, piece, hidden), half),
            pltpu.VMEM((SPLIT, rows, hidden), half),
            pltpu.VMEM((SPLIT, rows, hidden), half),
            pltpu.VMEM((SPLIT, rows, hidden), half),
            pltpu.VMEM((groups, SPLIT, piece, hidden), half),
            pltpu.VMEM((groups, SPLIT, piece, hidden), half),
            pltpu.VMEM((SPLIT, piece, hidden), half),
            pltpu.VMEM((SPLIT, piece, hidden), half),
            dma((9,)),
            dma((devices,)),
            dma((SPLIT,)),
            dma((groups,)),
            dma((SPLIT,)),
            dma((SPLIT, devices // ring)),
            dma((groups,)),
            dma((SPLIT,)),
        ],
        compiler_params=pltpu.CompilerParams(
            collective_id=0, has_side_effects=True, vmem_limit_bytes=48 * 1024 * 1024
        ),
    )(
        cotangent,
        expert_ids.reshape(1, tokens),
        route_weights.reshape(1, tokens),
        gate_pre,
        up_pre,
        down_weight,
    )


def solution(mesh):
    placed = (
        P(("dp", "expert"), None),
        P(("dp", "expert"), None),
        P(("dp", "expert"), None),
        P("dp", "expert"),
        P("dp", "expert"),
        P("dp", "expert"),
    )
    return jax.shard_map(
        per_device,
        mesh=mesh,
        in_specs=placed,
        out_specs=(P("dp", "expert"), P("dp", "expert"), P("dp", "expert")),
        check_vma=False,
    )
```

```python
import functools

import jax
import jax.numpy as jnp
from jax import lax
from jax.experimental import pallas as pl
from jax.experimental.pallas import tpu as pltpu
from jax.sharding import PartitionSpec as P

SPLIT = 4
ORDER = (0, 4, 1, 3, 7, 5, 2, 6)
MESH = pl.DeviceIdType.MESH


def fill_slots(groups, cotangent, ids, scales, ordered, sent):
    experts, _, quarters, lanes4, part = sent.shape
    tokens, width = cotangent.shape
    capacity = quarters * lanes4
    piece = part // groups
    lanes = 128 if part % 128 == 0 else part
    at = lax.broadcasted_iota(jnp.int32, (tokens, lanes), 1)
    for tile in range(width // lanes):
        whole = None
        lane = 0
        while lane < lanes:
            q, rest = divmod(tile * lanes + lane, part)
            i, t = divmod(rest, piece)
            source = i * SPLIT * piece + q * piece + t
            run = min(lanes - lane, piece - t, lanes - source % lanes)
            block = cotangent[:, source // lanes * lanes : (source // lanes + 1) * lanes]
            block = block.astype(jnp.float32)
            shift = (lane - source % lanes) % lanes
            if shift:
                block = pltpu.roll(block, shift, 1)
            whole = block if whole is None else jnp.where(at >= lane, block, whole)
            lane += run
        q, rest = divmod(tile * lanes, part)
        ordered[q, :, rest : rest + lanes] = whole.astype(jnp.bfloat16)

    names = ids[...]
    onehot = lax.broadcasted_iota(jnp.int32, (experts, tokens), 0) == names
    onehot = onehot.astype(jnp.float32)
    before = lax.broadcasted_iota(jnp.int32, (tokens, tokens), 0)
    before = before < lax.broadcasted_iota(jnp.int32, (tokens, tokens), 1)
    earlier = jnp.dot(
        onehot.astype(jnp.bfloat16),
        before.astype(jnp.float32).astype(jnp.bfloat16),
        preferred_element_type=jnp.float32,
    )
    position = jnp.sum(onehot * earlier, axis=0, keepdims=True)
    place = names.astype(jnp.float32) * capacity + position
    slots = lax.broadcasted_iota(jnp.int32, (experts * capacity, tokens), 0)
    picker = (slots.astype(jnp.float32) == place).astype(jnp.float32)
    slot_scale = jnp.sum(picker * scales[...], axis=1, keepdims=True)
    picker = picker.astype(jnp.bfloat16)
    for q in range(SPLIT):
        picked = jnp.dot(picker, ordered[q], preferred_element_type=jnp.float32)
        picked = (picked * slot_scale).astype(jnp.bfloat16)
        sent[:, q] = picked.reshape(experts, quarters, lanes4, part)


def wait_bytes(ref, sem):
    pltpu.make_async_copy(ref, ref, sem).wait()


def layer_kernel(
    dims,
    cotangent_hbm,
    ids,
    scales,
    gate_hbm,
    up_hbm,
    down_hbm,
    weight_grad,
    gate_grad,
    up_grad,
    cotangent,
    gate,
    up,
    down,
    ordered,
    sent,
    arrived,
    routed,
    own_weight,
    weight,
    products,
    partial,
    shares,
    grads,
    pair_parts,
    pairs,
    grad_parts,
    total,
    grad_rows,
    send_sems,
    token_sems,
    quad_weight_sems,
    weight_sems,
    product_sems,
    share_sems,
    grad_sems,
    total_sems,
    pair_sems,
    load_sems,
    plane_sem,
):
    groups, devices, ring = dims
    rows_y = devices // ring
    rows, hidden = gate.shape
    capacity = rows // devices
    chunk = rows // rows_y
    piece = down.shape[0] // SPLIT
    part = piece * groups
    i = lax.axis_index("dp")
    e = lax.axis_index("expert")
    y, z = e // ring, e % ring
    q = e % SPLIT
    base = e - q

    loads = [
        pltpu.make_async_copy(source, target, load_sems.at[at])
        for at, (source, target) in enumerate(
            ((gate_hbm, gate), (up_hbm, up), (cotangent_hbm, cotangent), (down_hbm, down))
        )
    ]
    for load in loads:
        load.start()

    def peer(target):
        return {"expert": target}

    barrier = pltpu.get_barrier_semaphore()

    @pl.loop(1, ring)
    def _(step):
        target = y * ring + lax.rem(z + step, ring)
        pl.semaphore_signal(barrier, inc=1, device_id=peer(target), device_id_type=MESH)

    @pl.loop(1, rows_y)
    def _(step):
        target = lax.rem(y + step, rows_y) * ring + z
        pl.semaphore_signal(barrier, inc=1, device_id=peer(target), device_id_type=MESH)

    @pl.loop(1, groups)
    def _(step):
        target = lax.rem(i + step, groups)
        pl.semaphore_signal(barrier, inc=1, device_id={"dp": target}, device_id_type=MESH)

    loads[0].wait()
    loads[1].wait()

    @pl.loop(0, rows_y)
    def _(step):
        span = pl.ds(pl.multiple_of(step * chunk, 16), chunk)
        g = gate[span, :].astype(jnp.float32)
        active = g / (1.0 + jnp.exp(-g))
        products[q, span, :] = (active * up[span, :].astype(jnp.float32)).astype(jnp.bfloat16)

    loads[3].wait()
    own_weight[q] = down[pl.ds(pl.multiple_of(q * piece, 16), piece), :]
    pl.semaphore_wait(barrier, ring - 1 + rows_y - 1 + groups - 1)

    @pl.loop(1, ring)
    def _(step):
        target = y * ring + lax.rem(z + step, ring)
        pl.semaphore_signal(plane_sem, inc=1, device_id=peer(target), device_id_type=MESH)


    for step in range(1, SPLIT):
        other = lax.rem(q + step, SPLIT)
        pltpu.make_async_remote_copy(
            src_ref=down.at[pl.ds(pl.multiple_of(other * piece, 16), piece)],
            dst_ref=own_weight.at[q],
            send_sem=send_sems.at[0],
            recv_sem=quad_weight_sems.at[q],
            device_id=peer(base + other),
            device_id_type=MESH,
        ).start()

    inner = (q == 1) | (q == 2)

    def product_to(block, other, stage):
        pltpu.make_async_remote_copy(
            src_ref=products.at[block],
            dst_ref=products.at[block],
            send_sem=send_sems.at[stage],
            recv_sem=product_sems.at[block],
            device_id=peer(base + other),
            device_id_type=MESH,
        ).start()

    @pl.when(q < SPLIT - 1)
    def _():
        product_to(q, q + 1, 3)

    @pl.when(q > 0)
    def _():
        product_to(q, q - 1, 3)

    loads[2].wait()
    fill_slots(groups, cotangent, ids, scales, ordered, sent)
    arrived[e] = sent[e // SPLIT, q]
    pl.semaphore_wait(plane_sem, ring - 1)

    def away(step, count):
        if count != 8:
            return step
        return sum(jnp.where(step == k, far, 0) for k, far in enumerate(ORDER))

    def send_tokens(first, last):
        @pl.loop(first * ring, last * ring)
        def _(step):
            to_y = lax.rem(y + away(step // ring, rows_y), rows_y)
            to_z = lax.rem(z + away(step % ring, ring), ring)
            target = to_y * ring + to_z

            @pl.when(target != e)
            def _():
                pltpu.make_async_remote_copy(
                    src_ref=sent.at[target // SPLIT, target % SPLIT],
                    dst_ref=arrived.at[e],
                    send_sem=send_sems.at[1],
                    recv_sem=token_sems.at[e],
                    device_id=peer(target),
                    device_id_type=MESH,
                ).start()

    send_tokens(0, rows_y // 2)

    for step in range(1, SPLIT):
        other = lax.rem(q + step, SPLIT)
        wait_bytes(own_weight.at[other], quad_weight_sems.at[other])
    weight[i] = own_weight[...]

    chips = groups // 2
    chip, core = i // 2, i % 2
    sibling = {"dp": chip * 2 + 1 - core}

    for hop in range(1, chips):
        pltpu.make_async_remote_copy(
            src_ref=weight.at[i],
            dst_ref=weight.at[i],
            send_sem=send_sems.at[2],
            recv_sem=weight_sems.at[i],
            device_id={"dp": lax.rem(chip + hop, chips) * 2 + core},
            device_id_type=MESH,
        ).start()

    def weight_over(block):
        pltpu.make_async_remote_copy(
            src_ref=weight.at[block],
            dst_ref=weight.at[block],
            send_sem=send_sems.at[9],
            recv_sem=weight_sems.at[block],
            device_id=sibling,
            device_id_type=MESH,
        ).start()

    weight_over(i)

    @pl.when(inner)
    def _():
        for way in (1, -1):
            wait_bytes(products.at[q - way], product_sems.at[q - way])
            product_to(q - way, q + way, 7)

    send_tokens(rows_y // 2, rows_y)
    far = jnp.where(q == 1, SPLIT - 1, 0)

    @pl.when(inner)
    def _():
        wait_bytes(products.at[far], product_sems.at[far])
        product_to(far, jnp.where(q == 1, 0, SPLIT - 1), 8)

    for hop in range(1, chips):
        source = lax.rem(chip + chips - hop, chips) * 2 + core
        wait_bytes(weight.at[source], weight_sems.at[source])
        weight_over(source)
    for hop in range(chips):
        source = lax.rem(chip + chips - hop, chips) * 2 + 1 - core
        wait_bytes(weight.at[source], weight_sems.at[source])

    @pl.loop(0, rows_y)
    def _(step):
        from_y = lax.rem(y + rows_y - lax.rem(away(step, rows_y), rows_y), rows_y)

        @pl.loop(0, ring)
        def _(at):
            source = from_y * ring + at

            @pl.when(source != e)
            def _():
                wait_bytes(arrived.at[source], token_sems.at[source])

        block = arrived[pl.ds(from_y * ring, ring)].reshape(chunk, part)
        span = pl.ds(pl.multiple_of(from_y * chunk, 16), chunk)
        routed[span, :] = block
        for j in range(SPLIT):
            partial[j, span, :] = jnp.dot(
                block, weight[:, j].reshape(part, hidden), preferred_element_type=jnp.float32
            ).astype(jnp.bfloat16)
        shares[q, span, :] = partial[q, span, :]
        for hop in range(1, SPLIT):
            other = lax.rem(q + hop, SPLIT)
            pltpu.make_async_remote_copy(
                src_ref=partial.at[other, span],
                dst_ref=shares.at[q, span],
                send_sem=send_sems.at[4],
                recv_sem=share_sems.at[q, from_y],
                device_id=peer(base + other),
                device_id_type=MESH,
            ).start()

    def slice_of(turn):
        j = jnp.where(turn == 3, q, jnp.where(q < 2, SPLIT - 1, 0))
        j = jnp.where(turn == 2, jnp.where(q < 2, 2, 1), j)
        return jnp.where(turn == 1, q + 1 - 2 * (q % 2), j)

    def pair_up(turn):
        j = slice_of(turn)
        wait_bytes(pair_parts.at[j], pair_sems.at[j])
        for at in range(chips):
            pair = grads[j, core, at].astype(jnp.float32)
            pair = pair + pair_parts[j, at].astype(jnp.float32)
            pairs[j, at] = pair.astype(jnp.bfloat16)
        grad_parts[j, chip] = pairs[j, chip]
        for hop in range(1, chips):
            target = lax.rem(chip + hop, chips)
            pltpu.make_async_remote_copy(
                src_ref=pairs.at[j, target],
                dst_ref=grad_parts.at[j, chip],
                send_sem=send_sems.at[5],
                recv_sem=grad_sems.at[j, chip],
                device_id={"dp": target * 2 + core},
                device_id_type=MESH,
            ).start()

    @pl.loop(1, SPLIT + 1)
    def _(turn):
        j = slice_of(turn)

        @pl.when((j != q) & jnp.logical_not(inner))
        def _():
            wait_bytes(products.at[j], product_sems.at[j])

        slice_grads = lax.dot_general(
            routed[...],
            products[j],
            (((0,), (0,)), ((), ())),
            preferred_element_type=jnp.float32,
        ).astype(jnp.bfloat16)
        for at in range(groups):
            grads[j, at % 2, at // 2] = slice_grads[at * piece : (at + 1) * piece]
        pltpu.make_async_remote_copy(
            src_ref=grads.at[j, 1 - core],
            dst_ref=pair_parts.at[j],
            send_sem=send_sems.at[10],
            recv_sem=pair_sems.at[j],
            device_id=sibling,
            device_id_type=MESH,
        ).start()

        @pl.when(turn > 1)
        def _():
            pair_up(turn - 1)

    pair_up(SPLIT)

    def finish(first, last):
        @pl.loop(first, last)
        def _(step):
            from_y = lax.rem(y + rows_y - lax.rem(away(step, rows_y), rows_y), rows_y)
            span = pl.ds(pl.multiple_of(from_y * chunk, 16), chunk)
            for hop in range(1, SPLIT):
                other = lax.rem(q + hop, SPLIT)
                wait_bytes(shares.at[other, span], share_sems.at[other, from_y])
            upstream = shares[0, span, :].astype(jnp.float32)
            for j in range(1, SPLIT):
                upstream = upstream + shares[j, span, :].astype(jnp.float32)
            g = gate[span, :].astype(jnp.float32)
            u = up[span, :].astype(jnp.float32)
            sigmoid = 1.0 / (1.0 + jnp.exp(-g))
            gate_grad[span, :] = (upstream * u * sigmoid * (1.0 + g * (1.0 - sigmoid))).astype(
                jnp.bfloat16
            )
            up_grad[span, :] = (upstream * (g * sigmoid)).astype(jnp.bfloat16)

    early = rows_y - rows_y // 4
    finish(0, early)

    @pl.loop(1, SPLIT + 1)
    def _(turn):
        j = slice_of(turn)
        for hop in range(1, chips):
            source = lax.rem(chip + hop, chips)
            wait_bytes(grad_parts.at[j, source], grad_sems.at[j, source])

        whole = grad_parts[j, 0].astype(jnp.float32)
        for k in range(1, chips):
            whole = whole + grad_parts[j, k].astype(jnp.float32)
        total[j] = whole.astype(jnp.bfloat16)

        @pl.when(j != q)
        def _():
            pltpu.make_async_remote_copy(
                src_ref=total.at[j],
                dst_ref=grad_rows.at[q],
                send_sem=send_sems.at[6],
                recv_sem=total_sems.at[q],
                device_id=peer(base + j),
                device_id_type=MESH,
            ).start()

    grad_rows[q] = total[q]
    finish(early, rows_y)
    for step in range(1, SPLIT):
        other = lax.rem(q + step, SPLIT)
        wait_bytes(grad_rows.at[other], total_sems.at[other])
    for j in range(SPLIT):
        weight_grad[j * piece : (j + 1) * piece, :] = grad_rows[j]

    wait_bytes(own_weight.at[pl.ds(0, SPLIT - 1)], send_sems.at[0])
    wait_bytes(arrived.at[pl.ds(0, devices - 1)], send_sems.at[1])
    if chips > 1:
        wait_bytes(weight.at[pl.ds(0, chips - 1)], send_sems.at[2])
        wait_bytes(pairs.at[:, pl.ds(0, chips - 1)], send_sems.at[5])
    wait_bytes(weight.at[pl.ds(0, chips)], send_sems.at[9])
    wait_bytes(pair_parts, send_sems.at[10])

    @pl.when(inner)
    def _():
        wait_bytes(products.at[pl.ds(0, 2)], send_sems.at[3])
        wait_bytes(products.at[pl.ds(0, 2)], send_sems.at[7])
        wait_bytes(products.at[0], send_sems.at[8])

    @pl.when(jnp.logical_not(inner))
    def _():
        wait_bytes(products.at[0], send_sems.at[3])

    wait_bytes(shares.at[pl.ds(0, SPLIT - 1)], send_sems.at[4])
    wait_bytes(total.at[pl.ds(0, SPLIT - 1)], send_sems.at[6])


def per_device(cotangent, expert_ids, route_weights, gate_pre, up_pre, down_weight):
    devices = lax.axis_size("expert")
    groups = lax.axis_size("dp")
    ring = 8 if devices == 64 else SPLIT
    experts = devices // SPLIT
    rows, hidden = gate_pre.shape
    capacity = rows // devices
    tokens, width = cotangent.shape
    part = width // SPLIT
    piece = part // groups

    half = jnp.bfloat16
    vmem = pl.BlockSpec(memory_space=pltpu.VMEM)
    hbm = pl.BlockSpec(memory_space=pl.ANY)
    dma = pltpu.SemaphoreType.DMA
    return pl.pallas_call(
        functools.partial(layer_kernel, (groups, devices, ring)),
        out_shape=(
            jax.ShapeDtypeStruct(down_weight.shape, half),
            jax.ShapeDtypeStruct(gate_pre.shape, half),
            jax.ShapeDtypeStruct(gate_pre.shape, half),
        ),
        in_specs=[hbm, vmem, vmem, hbm, hbm, hbm],
        out_specs=(vmem, vmem, vmem),
        scratch_shapes=[
            pltpu.VMEM((tokens, width), half),
            pltpu.VMEM((rows, hidden), half),
            pltpu.VMEM((rows, hidden), half),
            pltpu.VMEM(down_weight.shape, half),
            pltpu.VMEM((SPLIT, tokens, part), half),
            pltpu.VMEM((experts, SPLIT, capacity // 4, 4, part), half),
            pltpu.VMEM((devices, capacity // 4, 4, part), half),
            pltpu.VMEM((rows, part), half),
            pltpu.VMEM((SPLIT, piece, hidden), half),
            pltpu.VMEM((groups, SPLIT, piece, hidden), half),
            pltpu.VMEM((SPLIT, rows, hidden), half),
            pltpu.VMEM((SPLIT, rows, hidden), half),
            pltpu.VMEM((SPLIT, rows, hidden), half),
            pltpu.VMEM((SPLIT, 2, groups // 2, piece, hidden), half),
            pltpu.VMEM((SPLIT, groups // 2, piece, hidden), half),
            pltpu.VMEM((SPLIT, groups // 2, piece, hidden), half),
            pltpu.VMEM((SPLIT, groups // 2, piece, hidden), half),
            pltpu.VMEM((SPLIT, piece, hidden), half),
            pltpu.VMEM((SPLIT, piece, hidden), half),
            dma((11,)),
            dma((devices,)),
            dma((SPLIT,)),
            dma((groups,)),
            dma((SPLIT,)),
            dma((SPLIT, devices // ring)),
            dma((SPLIT, groups // 2)),
            dma((SPLIT,)),
            dma((SPLIT,)),
            dma((4,)),
            pltpu.SemaphoreType.REGULAR,
        ],
        compiler_params=pltpu.CompilerParams(
            collective_id=0, has_side_effects=True, vmem_limit_bytes=62 * 1024 * 1024
        ),
    )(
        cotangent,
        expert_ids.reshape(1, tokens),
        route_weights.reshape(1, tokens),
        gate_pre,
        up_pre,
        down_weight,
    )


def solution(mesh):
    placed = (
        P(("dp", "expert"), None),
        P(("dp", "expert"), None),
        P(("dp", "expert"), None),
        P("dp", "expert"),
        P("dp", "expert"),
        P("dp", "expert"),
    )
    return jax.shard_map(
        per_device,
        mesh=mesh,
        in_specs=placed,
        out_specs=(P("dp", "expert"), P("dp", "expert"), P("dp", "expert")),
        check_vma=False,
    )
```

```python
import functools

import jax
import jax.numpy as jnp
from jax import lax
from jax.experimental import pallas as pl
from jax.experimental.pallas import tpu as pltpu
from jax.sharding import PartitionSpec as P

SPLIT = 4
ORDER = (0, 4, 1, 3, 7, 5, 2, 6)
MESH = pl.DeviceIdType.MESH


def fill_slots(groups, cotangent, ids, scales, ordered, sent):
    experts, _, quarters, lanes4, part = sent.shape
    tokens, width = cotangent.shape
    capacity = quarters * lanes4
    piece = part // groups
    lanes = 128 if part % 128 == 0 else part
    at = lax.broadcasted_iota(jnp.int32, (tokens, lanes), 1)
    for tile in range(width // lanes):
        whole = None
        lane = 0
        while lane < lanes:
            q, rest = divmod(tile * lanes + lane, part)
            i, t = divmod(rest, piece)
            source = i * SPLIT * piece + q * piece + t
            run = min(lanes - lane, piece - t, lanes - source % lanes)
            block = cotangent[:, source // lanes * lanes : (source // lanes + 1) * lanes]
            block = block.astype(jnp.float32)
            shift = (lane - source % lanes) % lanes
            if shift:
                block = pltpu.roll(block, shift, 1)
            whole = block if whole is None else jnp.where(at >= lane, block, whole)
            lane += run
        q, rest = divmod(tile * lanes, part)
        ordered[q, :, rest : rest + lanes] = whole.astype(jnp.bfloat16)

    names = ids[...]
    onehot = lax.broadcasted_iota(jnp.int32, (experts, tokens), 0) == names
    onehot = onehot.astype(jnp.float32)
    before = lax.broadcasted_iota(jnp.int32, (tokens, tokens), 0)
    before = before < lax.broadcasted_iota(jnp.int32, (tokens, tokens), 1)
    earlier = jnp.dot(
        onehot.astype(jnp.bfloat16),
        before.astype(jnp.float32).astype(jnp.bfloat16),
        preferred_element_type=jnp.float32,
    )
    position = jnp.sum(onehot * earlier, axis=0, keepdims=True)
    place = names.astype(jnp.float32) * capacity + position
    slots = lax.broadcasted_iota(jnp.int32, (experts * capacity, tokens), 0)
    picker = (slots.astype(jnp.float32) == place).astype(jnp.float32)
    slot_scale = jnp.sum(picker * scales[...], axis=1, keepdims=True)
    picker = picker.astype(jnp.bfloat16)
    for q in range(SPLIT):
        picked = jnp.dot(picker, ordered[q], preferred_element_type=jnp.float32)
        picked = (picked * slot_scale).astype(jnp.bfloat16)
        sent[:, q] = picked.reshape(experts, quarters, lanes4, part)


def wait_bytes(ref, sem):
    pltpu.make_async_copy(ref, ref, sem).wait()


def layer_kernel(
    dims,
    cotangent_hbm,
    ids,
    scales,
    gate_hbm,
    up_hbm,
    down_hbm,
    weight_grad,
    gate_grad,
    up_grad,
    cotangent,
    gate,
    up,
    down,
    ordered,
    sent,
    arrived,
    routed,
    own_weight,
    weight,
    products,
    partial,
    shares,
    pass_in,
    grads,
    pair_parts,
    pairs,
    grad_parts,
    total,
    grad_rows,
    send_sems,
    token_sems,
    quad_weight_sems,
    weight_sems,
    product_sems,
    share_sems,
    grad_sems,
    total_sems,
    pair_sems,
    load_sems,
    plane_sem,
    pass_sems,
):
    groups, devices, ring = dims
    rows_y = devices // ring
    rows, hidden = gate.shape
    capacity = rows // devices
    chunk = rows // rows_y
    piece = down.shape[0] // SPLIT
    part = piece * groups
    i = lax.axis_index("dp")
    e = lax.axis_index("expert")
    y, z = e // ring, e % ring
    q = e % SPLIT
    base = e - q

    loads = [
        pltpu.make_async_copy(source, target, load_sems.at[at])
        for at, (source, target) in enumerate(
            ((gate_hbm, gate), (up_hbm, up), (cotangent_hbm, cotangent), (down_hbm, down))
        )
    ]
    for load in loads:
        load.start()

    def peer(target):
        return {"expert": target}

    barrier = pltpu.get_barrier_semaphore()

    @pl.loop(1, ring)
    def _(step):
        target = y * ring + lax.rem(z + step, ring)
        pl.semaphore_signal(barrier, inc=1, device_id=peer(target), device_id_type=MESH)

    @pl.loop(1, rows_y)
    def _(step):
        target = lax.rem(y + step, rows_y) * ring + z
        pl.semaphore_signal(barrier, inc=1, device_id=peer(target), device_id_type=MESH)

    @pl.loop(1, groups)
    def _(step):
        target = lax.rem(i + step, groups)
        pl.semaphore_signal(barrier, inc=1, device_id={"dp": target}, device_id_type=MESH)

    loads[0].wait()
    loads[1].wait()

    @pl.loop(0, rows_y)
    def _(step):
        span = pl.ds(pl.multiple_of(step * chunk, 16), chunk)
        g = gate[span, :].astype(jnp.float32)
        active = g / (1.0 + jnp.exp(-g))
        products[q, span, :] = (active * up[span, :].astype(jnp.float32)).astype(jnp.bfloat16)

    loads[3].wait()
    own_weight[q] = down[pl.ds(pl.multiple_of(q * piece, 16), piece), :]
    pl.semaphore_wait(barrier, ring - 1 + rows_y - 1 + groups - 1)

    @pl.loop(1, ring)
    def _(step):
        target = y * ring + lax.rem(z + step, ring)
        pl.semaphore_signal(plane_sem, inc=1, device_id=peer(target), device_id_type=MESH)


    for step in range(1, SPLIT):
        other = lax.rem(q + step, SPLIT)
        pltpu.make_async_remote_copy(
            src_ref=down.at[pl.ds(pl.multiple_of(other * piece, 16), piece)],
            dst_ref=own_weight.at[q],
            send_sem=send_sems.at[0],
            recv_sem=quad_weight_sems.at[q],
            device_id=peer(base + other),
            device_id_type=MESH,
        ).start()

    inner = (q == 1) | (q == 2)

    def product_to(block, other, stage):
        pltpu.make_async_remote_copy(
            src_ref=products.at[block],
            dst_ref=products.at[block],
            send_sem=send_sems.at[stage],
            recv_sem=product_sems.at[block],
            device_id=peer(base + other),
            device_id_type=MESH,
        ).start()

    @pl.when(q < SPLIT - 1)
    def _():
        product_to(q, q + 1, 3)

    @pl.when(q > 0)
    def _():
        product_to(q, q - 1, 3)

    loads[2].wait()
    fill_slots(groups, cotangent, ids, scales, ordered, sent)
    arrived[e] = sent[e // SPLIT, q]
    pl.semaphore_wait(plane_sem, ring - 1)

    def away(step, count):
        if count != 8:
            return step
        return sum(jnp.where(step == k, far, 0) for k, far in enumerate(ORDER))

    def send_tokens(first, last):
        @pl.loop(first * ring, last * ring)
        def _(step):
            to_y = lax.rem(y + away(step // ring, rows_y), rows_y)
            to_z = lax.rem(z + away(step % ring, ring), ring)
            target = to_y * ring + to_z

            @pl.when(target != e)
            def _():
                pltpu.make_async_remote_copy(
                    src_ref=sent.at[target // SPLIT, target % SPLIT],
                    dst_ref=arrived.at[e],
                    send_sem=send_sems.at[1],
                    recv_sem=token_sems.at[e],
                    device_id=peer(target),
                    device_id_type=MESH,
                ).start()

    send_tokens(0, rows_y // 2)

    for step in range(1, SPLIT):
        other = lax.rem(q + step, SPLIT)
        wait_bytes(own_weight.at[other], quad_weight_sems.at[other])
    weight[i] = own_weight[...]

    chips = groups // 2
    chip, core = i // 2, i % 2
    sibling = {"dp": chip * 2 + 1 - core}

    for hop in range(1, chips):
        pltpu.make_async_remote_copy(
            src_ref=weight.at[i],
            dst_ref=weight.at[i],
            send_sem=send_sems.at[2],
            recv_sem=weight_sems.at[i],
            device_id={"dp": lax.rem(chip + hop, chips) * 2 + core},
            device_id_type=MESH,
        ).start()

    def weight_over(block):
        pltpu.make_async_remote_copy(
            src_ref=weight.at[block],
            dst_ref=weight.at[block],
            send_sem=send_sems.at[9],
            recv_sem=weight_sems.at[block],
            device_id=sibling,
            device_id_type=MESH,
        ).start()

    weight_over(i)

    send_tokens(rows_y // 2, 3 * rows_y // 4)
    @pl.when(inner)
    def _():
        for way in (1, -1):
            wait_bytes(products.at[q - way], product_sems.at[q - way])
            product_to(q - way, q + way, 7)

    send_tokens(3 * rows_y // 4, rows_y)
    far = jnp.where(q == 1, SPLIT - 1, 0)

    @pl.when(inner)
    def _():
        wait_bytes(products.at[far], product_sems.at[far])
        product_to(far, jnp.where(q == 1, 0, SPLIT - 1), 8)

    for hop in range(1, chips):
        source = lax.rem(chip + chips - hop, chips) * 2 + core
        wait_bytes(weight.at[source], weight_sems.at[source])
        weight_over(source)
    for hop in range(chips):
        source = lax.rem(chip + chips - hop, chips) * 2 + 1 - core
        wait_bytes(weight.at[source], weight_sems.at[source])

    mate = q + 1 - 2 * (q % 2)
    fars = (jnp.where(q < 2, 2, 1), jnp.where(q < 2, SPLIT - 1, 0))

    def rows_of(step):
        from_y = lax.rem(y + rows_y - lax.rem(away(step, rows_y), rows_y), rows_y)
        return from_y, pl.ds(pl.multiple_of(from_y * chunk, 16), chunk)

    def share_to(source, target, stage, arrival, other):
        pltpu.make_async_remote_copy(
            src_ref=source,
            dst_ref=target,
            send_sem=send_sems.at[stage],
            recv_sem=arrival,
            device_id=peer(base + other),
            device_id_type=MESH,
        ).start()

    def pass_on(step):
        from_y, span = rows_of(step)
        for n in range(2):
            wait_bytes(pass_in.at[n, span], pass_sems.at[n, from_y])
            both = partial[fars[n], span, :].astype(jnp.float32)
            both = both + pass_in[n, span, :].astype(jnp.float32)
            partial[fars[n], span, :] = both.astype(jnp.bfloat16)
            share_to(partial.at[fars[n], span], shares.at[1, span], 12, share_sems.at[1, from_y], fars[n])

    @pl.loop(0, rows_y)
    def _(step):
        from_y = lax.rem(y + rows_y - lax.rem(away(step, rows_y), rows_y), rows_y)

        @pl.loop(0, ring)
        def _(at):
            source = from_y * ring + at

            @pl.when(source != e)
            def _():
                wait_bytes(arrived.at[source], token_sems.at[source])

        block = arrived[pl.ds(from_y * ring, ring)].reshape(chunk, part)
        span = pl.ds(pl.multiple_of(from_y * chunk, 16), chunk)
        routed[span, :] = block
        for j in range(SPLIT):
            partial[j, span, :] = jnp.dot(
                block, weight[:, j].reshape(part, hidden), preferred_element_type=jnp.float32
            ).astype(jnp.bfloat16)

        @pl.when(jnp.logical_not(inner))
        def _():
            for n in range(2):
                share_to(partial.at[fars[n], span], pass_in.at[n, span], 11, pass_sems.at[n, from_y], mate)

        share_to(partial.at[mate, span], shares.at[0, span], 4, share_sems.at[0, from_y], mate)

    def slice_of(turn):
        j = jnp.where(turn == 3, q, jnp.where(q < 2, SPLIT - 1, 0))
        j = jnp.where(turn == 2, jnp.where(q < 2, 2, 1), j)
        return jnp.where(turn == 1, q + 1 - 2 * (q % 2), j)

    def pair_up(turn):
        j = slice_of(turn)
        wait_bytes(pair_parts.at[j], pair_sems.at[j])
        for at in range(chips):
            pair = grads[j, core, at].astype(jnp.float32)
            pair = pair + pair_parts[j, at].astype(jnp.float32)
            pairs[j, at] = pair.astype(jnp.bfloat16)
        grad_parts[j, chip] = pairs[j, chip]
        for hop in range(1, chips):
            target = lax.rem(chip + hop, chips)
            pltpu.make_async_remote_copy(
                src_ref=pairs.at[j, target],
                dst_ref=grad_parts.at[j, chip],
                send_sem=send_sems.at[5],
                recv_sem=grad_sems.at[j, chip],
                device_id={"dp": target * 2 + core},
                device_id_type=MESH,
            ).start()

    @pl.loop(1, SPLIT + 1)
    def _(turn):
        j = slice_of(turn)

        @pl.when((j != q) & jnp.logical_not(inner))
        def _():
            wait_bytes(products.at[j], product_sems.at[j])

        slice_grads = lax.dot_general(
            routed[...],
            products[j],
            (((0,), (0,)), ((), ())),
            preferred_element_type=jnp.float32,
        ).astype(jnp.bfloat16)
        for at in range(groups):
            grads[j, at % 2, at // 2] = slice_grads[at * piece : (at + 1) * piece]
        pltpu.make_async_remote_copy(
            src_ref=grads.at[j, 1 - core],
            dst_ref=pair_parts.at[j],
            send_sem=send_sems.at[10],
            recv_sem=pair_sems.at[j],
            device_id=sibling,
            device_id_type=MESH,
        ).start()

        @pl.when(turn > 1)
        def _():
            pair_up(turn - 1)

        @pl.when(inner)
        def _():
            @pl.loop((turn - 1) * rows_y // 4, turn * rows_y // 4)
            def _(step):
                pass_on(step)

    pair_up(SPLIT)

    def finish(first, last):
        @pl.loop(first, last)
        def _(step):
            from_y = lax.rem(y + rows_y - lax.rem(away(step, rows_y), rows_y), rows_y)
            span = pl.ds(pl.multiple_of(from_y * chunk, 16), chunk)
            upstream = partial[q, span, :].astype(jnp.float32)
            for n in range(2):
                wait_bytes(shares.at[n, span], share_sems.at[n, from_y])
                upstream = upstream + shares[n, span, :].astype(jnp.float32)
            g = gate[span, :].astype(jnp.float32)
            u = up[span, :].astype(jnp.float32)
            sigmoid = 1.0 / (1.0 + jnp.exp(-g))
            gate_grad[span, :] = (upstream * u * sigmoid * (1.0 + g * (1.0 - sigmoid))).astype(
                jnp.bfloat16
            )
            up_grad[span, :] = (upstream * (g * sigmoid)).astype(jnp.bfloat16)

    early = rows_y - rows_y // 4
    finish(0, early)

    @pl.loop(1, SPLIT + 1)
    def _(turn):
        j = slice_of(turn)
        for hop in range(1, chips):
            source = lax.rem(chip + hop, chips)
            wait_bytes(grad_parts.at[j, source], grad_sems.at[j, source])

        whole = grad_parts[j, 0].astype(jnp.float32)
        for k in range(1, chips):
            whole = whole + grad_parts[j, k].astype(jnp.float32)
        total[j] = whole.astype(jnp.bfloat16)

        @pl.when(j != q)
        def _():
            pltpu.make_async_remote_copy(
                src_ref=total.at[j],
                dst_ref=grad_rows.at[q],
                send_sem=send_sems.at[6],
                recv_sem=total_sems.at[q],
                device_id=peer(base + j),
                device_id_type=MESH,
            ).start()

    grad_rows[q] = total[q]
    finish(early, rows_y)
    for step in range(1, SPLIT):
        other = lax.rem(q + step, SPLIT)
        wait_bytes(grad_rows.at[other], total_sems.at[other])
    for j in range(SPLIT):
        weight_grad[j * piece : (j + 1) * piece, :] = grad_rows[j]

    wait_bytes(own_weight.at[pl.ds(0, SPLIT - 1)], send_sems.at[0])
    wait_bytes(arrived.at[pl.ds(0, devices - 1)], send_sems.at[1])
    if chips > 1:
        wait_bytes(weight.at[pl.ds(0, chips - 1)], send_sems.at[2])
        wait_bytes(pairs.at[:, pl.ds(0, chips - 1)], send_sems.at[5])
    wait_bytes(weight.at[pl.ds(0, chips)], send_sems.at[9])
    wait_bytes(pair_parts, send_sems.at[10])

    @pl.when(inner)
    def _():
        wait_bytes(products.at[pl.ds(0, 2)], send_sems.at[3])
        wait_bytes(products.at[pl.ds(0, 2)], send_sems.at[7])
        wait_bytes(products.at[0], send_sems.at[8])

    @pl.when(jnp.logical_not(inner))
    def _():
        wait_bytes(products.at[0], send_sems.at[3])

    wait_bytes(shares.at[0], send_sems.at[4])

    @pl.when(inner)
    def _():
        wait_bytes(shares, send_sems.at[12])

    @pl.when(jnp.logical_not(inner))
    def _():
        wait_bytes(shares, send_sems.at[11])

    wait_bytes(total.at[pl.ds(0, SPLIT - 1)], send_sems.at[6])


def per_device(cotangent, expert_ids, route_weights, gate_pre, up_pre, down_weight):
    devices = lax.axis_size("expert")
    groups = lax.axis_size("dp")
    ring = 8 if devices == 64 else SPLIT
    experts = devices // SPLIT
    rows, hidden = gate_pre.shape
    capacity = rows // devices
    tokens, width = cotangent.shape
    part = width // SPLIT
    piece = part // groups

    half = jnp.bfloat16
    vmem = pl.BlockSpec(memory_space=pltpu.VMEM)
    hbm = pl.BlockSpec(memory_space=pl.ANY)
    dma = pltpu.SemaphoreType.DMA
    return pl.pallas_call(
        functools.partial(layer_kernel, (groups, devices, ring)),
        out_shape=(
            jax.ShapeDtypeStruct(down_weight.shape, half),
            jax.ShapeDtypeStruct(gate_pre.shape, half),
            jax.ShapeDtypeStruct(gate_pre.shape, half),
        ),
        in_specs=[hbm, vmem, vmem, hbm, hbm, hbm],
        out_specs=(vmem, vmem, vmem),
        scratch_shapes=[
            pltpu.VMEM((tokens, width), half),
            pltpu.VMEM((rows, hidden), half),
            pltpu.VMEM((rows, hidden), half),
            pltpu.VMEM(down_weight.shape, half),
            pltpu.VMEM((SPLIT, tokens, part), half),
            pltpu.VMEM((experts, SPLIT, capacity // 4, 4, part), half),
            pltpu.VMEM((devices, capacity // 4, 4, part), half),
            pltpu.VMEM((rows, part), half),
            pltpu.VMEM((SPLIT, piece, hidden), half),
            pltpu.VMEM((groups, SPLIT, piece, hidden), half),
            pltpu.VMEM((SPLIT, rows, hidden), half),
            pltpu.VMEM((SPLIT, rows, hidden), half),
            pltpu.VMEM((2, rows, hidden), half),
            pltpu.VMEM((2, rows, hidden), half),
            pltpu.VMEM((SPLIT, 2, groups // 2, piece, hidden), half),
            pltpu.VMEM((SPLIT, groups // 2, piece, hidden), half),
            pltpu.VMEM((SPLIT, groups // 2, piece, hidden), half),
            pltpu.VMEM((SPLIT, groups // 2, piece, hidden), half),
            pltpu.VMEM((SPLIT, piece, hidden), half),
            pltpu.VMEM((SPLIT, piece, hidden), half),
            dma((13,)),
            dma((devices,)),
            dma((SPLIT,)),
            dma((groups,)),
            dma((SPLIT,)),
            dma((2, devices // ring)),
            dma((SPLIT, groups // 2)),
            dma((SPLIT,)),
            dma((SPLIT,)),
            dma((4,)),
            pltpu.SemaphoreType.REGULAR,
            dma((2, devices // ring)),
        ],
        compiler_params=pltpu.CompilerParams(
            collective_id=0, has_side_effects=True, vmem_limit_bytes=62 * 1024 * 1024
        ),
    )(
        cotangent,
        expert_ids.reshape(1, tokens),
        route_weights.reshape(1, tokens),
        gate_pre,
        up_pre,
        down_weight,
    )


def solution(mesh):
    placed = (
        P(("dp", "expert"), None),
        P(("dp", "expert"), None),
        P(("dp", "expert"), None),
        P("dp", "expert"),
        P("dp", "expert"),
        P("dp", "expert"),
    )
    return jax.shard_map(
        per_device,
        mesh=mesh,
        in_specs=placed,
        out_specs=(P("dp", "expert"), P("dp", "expert"), P("dp", "expert")),
        check_vma=False,
    )
```

```python
import functools

import jax
import jax.numpy as jnp
from jax import lax
from jax.experimental import pallas as pl
from jax.experimental.pallas import tpu as pltpu
from jax.sharding import PartitionSpec as P

SPLIT = 4
ORDER = (0, 4, 1, 3, 7, 5, 2, 6)
MESH = pl.DeviceIdType.MESH


def fill_slots(groups, cotangent, ids, scales, ordered, sent):
    experts, _, quarters, lanes4, part = sent.shape
    tokens, width = cotangent.shape
    capacity = quarters * lanes4
    piece = part // groups
    lanes = 128 if part % 128 == 0 else part
    at = lax.broadcasted_iota(jnp.int32, (tokens, lanes), 1)
    for tile in range(width // lanes):
        whole = None
        lane = 0
        while lane < lanes:
            q, rest = divmod(tile * lanes + lane, part)
            i, t = divmod(rest, piece)
            source = i * SPLIT * piece + q * piece + t
            run = min(lanes - lane, piece - t, lanes - source % lanes)
            block = cotangent[:, source // lanes * lanes : (source // lanes + 1) * lanes]
            block = block.astype(jnp.float32)
            shift = (lane - source % lanes) % lanes
            if shift:
                block = pltpu.roll(block, shift, 1)
            whole = block if whole is None else jnp.where(at >= lane, block, whole)
            lane += run
        q, rest = divmod(tile * lanes, part)
        ordered[q, :, rest : rest + lanes] = whole.astype(jnp.bfloat16)

    names = ids[...]
    onehot = lax.broadcasted_iota(jnp.int32, (experts, tokens), 0) == names
    onehot = onehot.astype(jnp.float32)
    before = lax.broadcasted_iota(jnp.int32, (tokens, tokens), 0)
    before = before < lax.broadcasted_iota(jnp.int32, (tokens, tokens), 1)
    earlier = jnp.dot(
        onehot.astype(jnp.bfloat16),
        before.astype(jnp.float32).astype(jnp.bfloat16),
        preferred_element_type=jnp.float32,
    )
    position = jnp.sum(onehot * earlier, axis=0, keepdims=True)
    place = names.astype(jnp.float32) * capacity + position
    slots = lax.broadcasted_iota(jnp.int32, (experts * capacity, tokens), 0)
    picker = (slots.astype(jnp.float32) == place).astype(jnp.float32)
    slot_scale = jnp.sum(picker * scales[...], axis=1, keepdims=True)
    picker = picker.astype(jnp.bfloat16)
    for q in range(SPLIT):
        picked = jnp.dot(picker, ordered[q], preferred_element_type=jnp.float32)
        picked = (picked * slot_scale).astype(jnp.bfloat16)
        sent[:, q] = picked.reshape(experts, quarters, lanes4, part)


def wait_bytes(ref, sem):
    pltpu.make_async_copy(ref, ref, sem).wait()


def layer_kernel(
    dims,
    cotangent_hbm,
    ids,
    scales,
    gate_hbm,
    up_hbm,
    down_hbm,
    weight_grad,
    gate_grad,
    up_grad,
    cotangent,
    gate,
    up,
    down,
    ordered,
    sent,
    arrived,
    routed,
    own_weight,
    weight,
    products,
    partial,
    shares,
    pass_in,
    grads,
    pair_parts,
    pairs,
    grad_parts,
    total,
    grad_rows,
    send_sems,
    token_sems,
    quad_weight_sems,
    weight_sems,
    product_sems,
    share_sems,
    grad_sems,
    total_sems,
    pair_sems,
    load_sems,
    plane_sem,
    pass_sems,
):
    groups, devices, ring = dims
    rows_y = devices // ring
    rows, hidden = gate.shape
    capacity = rows // devices
    chunk = rows // rows_y
    piece = down.shape[0] // SPLIT
    part = piece * groups
    i = lax.axis_index("dp")
    e = lax.axis_index("expert")
    y, z = e // ring, e % ring
    q = e % SPLIT
    base = e - q

    loads = [
        pltpu.make_async_copy(source, target, load_sems.at[at])
        for at, (source, target) in enumerate(
            ((gate_hbm, gate), (up_hbm, up), (cotangent_hbm, cotangent), (down_hbm, down))
        )
    ]
    for load in loads:
        load.start()

    def peer(target):
        return {"expert": target}

    barrier = pltpu.get_barrier_semaphore()

    @pl.loop(1, ring)
    def _(step):
        target = y * ring + lax.rem(z + step, ring)
        pl.semaphore_signal(barrier, inc=1, device_id=peer(target), device_id_type=MESH)

    @pl.loop(1, rows_y)
    def _(step):
        target = lax.rem(y + step, rows_y) * ring + z
        pl.semaphore_signal(barrier, inc=1, device_id=peer(target), device_id_type=MESH)

    @pl.loop(1, groups)
    def _(step):
        target = lax.rem(i + step, groups)
        pl.semaphore_signal(barrier, inc=1, device_id={"dp": target}, device_id_type=MESH)

    loads[0].wait()
    loads[1].wait()

    @pl.loop(0, rows_y)
    def _(step):
        span = pl.ds(pl.multiple_of(step * chunk, 16), chunk)
        g = gate[span, :].astype(jnp.float32)
        active = g / (1.0 + jnp.exp(-g))
        products[q, span, :] = (active * up[span, :].astype(jnp.float32)).astype(jnp.bfloat16)

    loads[3].wait()
    own_weight[q] = down[pl.ds(pl.multiple_of(q * piece, 16), piece), :]
    pl.semaphore_wait(barrier, ring - 1 + rows_y - 1 + groups - 1)

    @pl.loop(1, ring)
    def _(step):
        target = y * ring + lax.rem(z + step, ring)
        pl.semaphore_signal(plane_sem, inc=1, device_id=peer(target), device_id_type=MESH)


    for step in range(1, SPLIT):
        other = lax.rem(q + step, SPLIT)
        pltpu.make_async_remote_copy(
            src_ref=down.at[pl.ds(pl.multiple_of(other * piece, 16), piece)],
            dst_ref=own_weight.at[q],
            send_sem=send_sems.at[0],
            recv_sem=quad_weight_sems.at[q],
            device_id=peer(base + other),
            device_id_type=MESH,
        ).start()

    inner = (q == 1) | (q == 2)

    def product_to(block, other, stage):
        pltpu.make_async_remote_copy(
            src_ref=products.at[block],
            dst_ref=products.at[block],
            send_sem=send_sems.at[stage],
            recv_sem=product_sems.at[block],
            device_id=peer(base + other),
            device_id_type=MESH,
        ).start()

    @pl.when(q < SPLIT - 1)
    def _():
        product_to(q, q + 1, 3)

    @pl.when(q > 0)
    def _():
        product_to(q, q - 1, 3)

    loads[2].wait()
    fill_slots(groups, cotangent, ids, scales, ordered, sent)
    arrived[e] = sent[e // SPLIT, q]
    pl.semaphore_wait(plane_sem, ring - 1)

    def away(step, count):
        if count != 8:
            return step
        return sum(jnp.where(step == k, far, 0) for k, far in enumerate(ORDER))

    def send_tokens(first, last):
        @pl.loop(first * ring, last * ring)
        def _(step):
            to_y = lax.rem(y + away(step // ring, rows_y), rows_y)
            to_z = lax.rem(z + away(step % ring, ring), ring)
            target = to_y * ring + to_z

            @pl.when(target != e)
            def _():
                pltpu.make_async_remote_copy(
                    src_ref=sent.at[target // SPLIT, target % SPLIT],
                    dst_ref=arrived.at[e],
                    send_sem=send_sems.at[1],
                    recv_sem=token_sems.at[e],
                    device_id=peer(target),
                    device_id_type=MESH,
                ).start()

    send_tokens(0, rows_y // 2)

    for step in range(1, SPLIT):
        other = lax.rem(q + step, SPLIT)
        wait_bytes(own_weight.at[other], quad_weight_sems.at[other])
    weight[i] = own_weight[...]

    chips = groups // 2
    chip, core = i // 2, i % 2
    sibling = {"dp": chip * 2 + 1 - core}

    for hop in range(1, chips):
        pltpu.make_async_remote_copy(
            src_ref=weight.at[i],
            dst_ref=weight.at[i],
            send_sem=send_sems.at[2],
            recv_sem=weight_sems.at[i],
            device_id={"dp": lax.rem(chip + hop, chips) * 2 + core},
            device_id_type=MESH,
        ).start()

    def weight_over(block):
        pltpu.make_async_remote_copy(
            src_ref=weight.at[block],
            dst_ref=weight.at[block],
            send_sem=send_sems.at[9],
            recv_sem=weight_sems.at[block],
            device_id=sibling,
            device_id_type=MESH,
        ).start()

    weight_over(i)

    send_tokens(rows_y // 2, 3 * rows_y // 4)
    send_tokens(3 * rows_y // 4, rows_y)
    @pl.when(inner)
    def _():
        for way in (1, -1):
            wait_bytes(products.at[q - way], product_sems.at[q - way])
            product_to(q - way, q + way, 7)

    far = jnp.where(q == 1, SPLIT - 1, 0)

    @pl.when(inner)
    def _():
        wait_bytes(products.at[far], product_sems.at[far])
        product_to(far, jnp.where(q == 1, 0, SPLIT - 1), 8)

    for hop in range(1, chips):
        source = lax.rem(chip + chips - hop, chips) * 2 + core
        wait_bytes(weight.at[source], weight_sems.at[source])
        weight_over(source)
    for hop in range(chips):
        source = lax.rem(chip + chips - hop, chips) * 2 + 1 - core
        wait_bytes(weight.at[source], weight_sems.at[source])

    mate = q + 1 - 2 * (q % 2)
    fars = (jnp.where(q < 2, 2, 1), jnp.where(q < 2, SPLIT - 1, 0))

    def rows_of(step):
        from_y = lax.rem(y + rows_y - lax.rem(away(step, rows_y), rows_y), rows_y)
        return from_y, pl.ds(pl.multiple_of(from_y * chunk, 16), chunk)

    def share_to(source, target, stage, arrival, other):
        pltpu.make_async_remote_copy(
            src_ref=source,
            dst_ref=target,
            send_sem=send_sems.at[stage],
            recv_sem=arrival,
            device_id=peer(base + other),
            device_id_type=MESH,
        ).start()

    def pass_on(step):
        from_y, span = rows_of(step)
        for n in range(2):
            wait_bytes(pass_in.at[n, span], pass_sems.at[n, from_y])
            both = partial[fars[n], span, :].astype(jnp.float32)
            both = both + pass_in[n, span, :].astype(jnp.float32)
            partial[fars[n], span, :] = both.astype(jnp.bfloat16)
            share_to(partial.at[fars[n], span], shares.at[1, span], 12, share_sems.at[1, from_y], fars[n])

    @pl.loop(0, rows_y)
    def _(step):
        from_y = lax.rem(y + rows_y - lax.rem(away(step, rows_y), rows_y), rows_y)

        @pl.loop(0, ring)
        def _(at):
            source = from_y * ring + at

            @pl.when(source != e)
            def _():
                wait_bytes(arrived.at[source], token_sems.at[source])

        block = arrived[pl.ds(from_y * ring, ring)].reshape(chunk, part)
        span = pl.ds(pl.multiple_of(from_y * chunk, 16), chunk)
        routed[span, :] = block
        for j in range(SPLIT):
            partial[j, span, :] = jnp.dot(
                block, weight[:, j].reshape(part, hidden), preferred_element_type=jnp.float32
            ).astype(jnp.bfloat16)

        @pl.when(jnp.logical_not(inner))
        def _():
            for n in range(2):
                share_to(partial.at[fars[n], span], pass_in.at[n, span], 11, pass_sems.at[n, from_y], mate)

        share_to(partial.at[mate, span], shares.at[0, span], 4, share_sems.at[0, from_y], mate)

    def slice_of(turn):
        j = jnp.where(turn == 3, q, jnp.where(q < 2, SPLIT - 1, 0))
        j = jnp.where(turn == 2, jnp.where(q < 2, 2, 1), j)
        return jnp.where(turn == 1, q + 1 - 2 * (q % 2), j)

    def pair_up(turn):
        j = slice_of(turn)
        wait_bytes(pair_parts.at[j], pair_sems.at[j])
        for at in range(chips):
            pair = grads[j, core, at].astype(jnp.float32)
            pair = pair + pair_parts[j, at].astype(jnp.float32)
            pairs[j, at] = pair.astype(jnp.bfloat16)
        grad_parts[j, chip] = pairs[j, chip]
        for hop in range(1, chips):
            target = lax.rem(chip + hop, chips)
            pltpu.make_async_remote_copy(
                src_ref=pairs.at[j, target],
                dst_ref=grad_parts.at[j, chip],
                send_sem=send_sems.at[5],
                recv_sem=grad_sems.at[j, chip],
                device_id={"dp": target * 2 + core},
                device_id_type=MESH,
            ).start()

    @pl.loop(1, SPLIT + 1)
    def _(turn):
        j = slice_of(turn)

        @pl.when((j != q) & jnp.logical_not(inner))
        def _():
            wait_bytes(products.at[j], product_sems.at[j])

        slice_grads = lax.dot_general(
            routed[...],
            products[j],
            (((0,), (0,)), ((), ())),
            preferred_element_type=jnp.float32,
        ).astype(jnp.bfloat16)
        for at in range(groups):
            grads[j, at % 2, at // 2] = slice_grads[at * piece : (at + 1) * piece]
        pltpu.make_async_remote_copy(
            src_ref=grads.at[j, 1 - core],
            dst_ref=pair_parts.at[j],
            send_sem=send_sems.at[10],
            recv_sem=pair_sems.at[j],
            device_id=sibling,
            device_id_type=MESH,
        ).start()

        @pl.when(turn > 1)
        def _():
            pair_up(turn - 1)

        @pl.when(inner)
        def _():
            @pl.loop((turn - 1) * rows_y // 4, turn * rows_y // 4)
            def _(step):
                pass_on(step)

    pair_up(SPLIT)

    def finish(first, last):
        @pl.loop(first, last)
        def _(step):
            from_y = lax.rem(y + rows_y - lax.rem(away(step, rows_y), rows_y), rows_y)
            span = pl.ds(pl.multiple_of(from_y * chunk, 16), chunk)
            upstream = partial[q, span, :].astype(jnp.float32)
            for n in range(2):
                wait_bytes(shares.at[n, span], share_sems.at[n, from_y])
                upstream = upstream + shares[n, span, :].astype(jnp.float32)
            g = gate[span, :].astype(jnp.float32)
            u = up[span, :].astype(jnp.float32)
            sigmoid = 1.0 / (1.0 + jnp.exp(-g))
            gate_grad[span, :] = (upstream * u * sigmoid * (1.0 + g * (1.0 - sigmoid))).astype(
                jnp.bfloat16
            )
            up_grad[span, :] = (upstream * (g * sigmoid)).astype(jnp.bfloat16)

    early = rows_y // 4
    finish(0, early)

    @pl.loop(1, SPLIT + 1)
    def _(turn):
        j = slice_of(turn)
        for hop in range(1, chips):
            source = lax.rem(chip + hop, chips)
            wait_bytes(grad_parts.at[j, source], grad_sems.at[j, source])

        whole = grad_parts[j, 0].astype(jnp.float32)
        for k in range(1, chips):
            whole = whole + grad_parts[j, k].astype(jnp.float32)
        total[j] = whole.astype(jnp.bfloat16)

        @pl.when(j != q)
        def _():
            pltpu.make_async_remote_copy(
                src_ref=total.at[j],
                dst_ref=grad_rows.at[q],
                send_sem=send_sems.at[6],
                recv_sem=total_sems.at[q],
                device_id=peer(base + j),
                device_id_type=MESH,
            ).start()

    grad_rows[q] = total[q]
    finish(early, rows_y)
    for step in range(1, SPLIT):
        other = lax.rem(q + step, SPLIT)
        wait_bytes(grad_rows.at[other], total_sems.at[other])
    for j in range(SPLIT):
        weight_grad[j * piece : (j + 1) * piece, :] = grad_rows[j]

    wait_bytes(own_weight.at[pl.ds(0, SPLIT - 1)], send_sems.at[0])
    wait_bytes(arrived.at[pl.ds(0, devices - 1)], send_sems.at[1])
    if chips > 1:
        wait_bytes(weight.at[pl.ds(0, chips - 1)], send_sems.at[2])
        wait_bytes(pairs.at[:, pl.ds(0, chips - 1)], send_sems.at[5])
    wait_bytes(weight.at[pl.ds(0, chips)], send_sems.at[9])
    wait_bytes(pair_parts, send_sems.at[10])

    @pl.when(inner)
    def _():
        wait_bytes(products.at[pl.ds(0, 2)], send_sems.at[3])
        wait_bytes(products.at[pl.ds(0, 2)], send_sems.at[7])
        wait_bytes(products.at[0], send_sems.at[8])

    @pl.when(jnp.logical_not(inner))
    def _():
        wait_bytes(products.at[0], send_sems.at[3])

    wait_bytes(shares.at[0], send_sems.at[4])

    @pl.when(inner)
    def _():
        wait_bytes(shares, send_sems.at[12])

    @pl.when(jnp.logical_not(inner))
    def _():
        wait_bytes(shares, send_sems.at[11])

    wait_bytes(total.at[pl.ds(0, SPLIT - 1)], send_sems.at[6])


def per_device(cotangent, expert_ids, route_weights, gate_pre, up_pre, down_weight):
    devices = lax.axis_size("expert")
    groups = lax.axis_size("dp")
    ring = 8 if devices == 64 else SPLIT
    experts = devices // SPLIT
    rows, hidden = gate_pre.shape
    capacity = rows // devices
    tokens, width = cotangent.shape
    part = width // SPLIT
    piece = part // groups

    half = jnp.bfloat16
    vmem = pl.BlockSpec(memory_space=pltpu.VMEM)
    hbm = pl.BlockSpec(memory_space=pl.ANY)
    dma = pltpu.SemaphoreType.DMA
    return pl.pallas_call(
        functools.partial(layer_kernel, (groups, devices, ring)),
        out_shape=(
            jax.ShapeDtypeStruct(down_weight.shape, half),
            jax.ShapeDtypeStruct(gate_pre.shape, half),
            jax.ShapeDtypeStruct(gate_pre.shape, half),
        ),
        in_specs=[hbm, vmem, vmem, hbm, hbm, hbm],
        out_specs=(vmem, vmem, vmem),
        scratch_shapes=[
            pltpu.VMEM((tokens, width), half),
            pltpu.VMEM((rows, hidden), half),
            pltpu.VMEM((rows, hidden), half),
            pltpu.VMEM(down_weight.shape, half),
            pltpu.VMEM((SPLIT, tokens, part), half),
            pltpu.VMEM((experts, SPLIT, capacity // 4, 4, part), half),
            pltpu.VMEM((devices, capacity // 4, 4, part), half),
            pltpu.VMEM((rows, part), half),
            pltpu.VMEM((SPLIT, piece, hidden), half),
            pltpu.VMEM((groups, SPLIT, piece, hidden), half),
            pltpu.VMEM((SPLIT, rows, hidden), half),
            pltpu.VMEM((SPLIT, rows, hidden), half),
            pltpu.VMEM((2, rows, hidden), half),
            pltpu.VMEM((2, rows, hidden), half),
            pltpu.VMEM((SPLIT, 2, groups // 2, piece, hidden), half),
            pltpu.VMEM((SPLIT, groups // 2, piece, hidden), half),
            pltpu.VMEM((SPLIT, groups // 2, piece, hidden), half),
            pltpu.VMEM((SPLIT, groups // 2, piece, hidden), half),
            pltpu.VMEM((SPLIT, piece, hidden), half),
            pltpu.VMEM((SPLIT, piece, hidden), half),
            dma((13,)),
            dma((devices,)),
            dma((SPLIT,)),
            dma((groups,)),
            dma((SPLIT,)),
            dma((2, devices // ring)),
            dma((SPLIT, groups // 2)),
            dma((SPLIT,)),
            dma((SPLIT,)),
            dma((4,)),
            pltpu.SemaphoreType.REGULAR,
            dma((2, devices // ring)),
        ],
        compiler_params=pltpu.CompilerParams(
            collective_id=0, has_side_effects=True, vmem_limit_bytes=62 * 1024 * 1024
        ),
    )(
        cotangent,
        expert_ids.reshape(1, tokens),
        route_weights.reshape(1, tokens),
        gate_pre,
        up_pre,
        down_weight,
    )


def solution(mesh):
    placed = (
        P(("dp", "expert"), None),
        P(("dp", "expert"), None),
        P(("dp", "expert"), None),
        P("dp", "expert"),
        P("dp", "expert"),
        P("dp", "expert"),
    )
    return jax.shard_map(
        per_device,
        mesh=mesh,
        in_specs=placed,
        out_specs=(P("dp", "expert"), P("dp", "expert"), P("dp", "expert")),
        check_vma=False,
    )
```
